512 devices in a mesh: dp: 32 (over x, y), tensor: 16 (over z, core).
Axes of the slice: x: 4, y: 8, z: 8, core: 2. Of those that a mesh axis runs over, the one named last changes fastest.
Arguments:
- queries: bfloat16 [4096, 16384], P('dp', 'tensor'), may hold values from -24 to 24
- draft_keys: bfloat16 [4096, 1024], P('dp'), may hold values from -6 to 6
- draft_values: bfloat16 [4096, 1024], P('dp'), may hold values from -6 to 6
- cache_keys: bfloat16 [64, 2048, 1024], P('dp', 'tensor'), may hold values from -24 to 24
- cache_values: bfloat16 [64, 2048, 1024], P('dp', 'tensor'), may hold values from -6 to 6
- out_weight: bfloat16 [16384, 16384], P('tensor', 'dp'), may hold values from -0.25 to 0.25
- cache_lengths: int32 [64], P('dp'), may hold values from 512 to 2048
- draft_lengths: int32 [64], replicated, may hold values from 8 to 64
- dest_group: int32 [64], replicated, may hold values from 0 to 31, as said below
- dest_offset: int32 [64], replicated, may hold values from 0 to 32, as said below
Outputs:
- verified: bfloat16 [3072, 16384], P('tensor', 'dp')
The draws below stay inside these ranges and needn't reach their ends.
Inputs may be any that keep to these rules, and one draw needn't show every extreme that they name: `dest_group`: at most one request of a group has another group as destination, and each group receives at most one such request. `dest_offset`: blocks with the same destination never intersect and end at packed row 96 or before; a block moved to another group starts right after that group's own rows; in every draw some group's blocks fill all 96 rows.
All inputs are finite; a program needn't handle non-finite values.
Results may differ from the reference program's by a relative error of at most 0.017.
Values may be sent and summed in bfloat16 or wider, within the bound.
No kernel may reach another device: no remote copies, remote signals or barrier semaphores. Data moves between devices by JAX's collectives and lax.ppermute only.
A program may use at most 64 MiB of HBM per device.

```python
import jax
import jax.numpy as jnp
from jax import lax

MODEL_DIM = 16384
HEADS = 128
KV_HEADS = 8
HEAD_DIM = 128
DRAFT = 64
GROUP_REQ = 2
CACHE = 2048
PACK = 96
REQUESTS = 64
TOKENS = 4096
ROWS = 3072
N_TENSOR = 16


def draw_queries(key, part):
    base_draw = 2.0 * jnp.clip(jax.random.normal(jax.random.fold_in(key, 1), (TOKENS, HEADS * HEAD_DIM), jnp.float32), -6.0, 6.0)
    return jnp.clip(base_draw, -24.0, 24.0).astype(jnp.bfloat16)


def draw_cache_keys(key, part):
    base_draw = jnp.clip(jax.random.normal(jax.random.fold_in(key, 3), (REQUESTS, CACHE, KV_HEADS * HEAD_DIM), jnp.float32), -6.0, 6.0)
    return jnp.clip(base_draw, -24.0, 24.0).astype(jnp.bfloat16)


def plan_tables(key):
    groups = REQUESTS // GROUP_REQ
    half_count = groups // 2
    group_order = jax.random.permutation(jax.random.fold_in(key, 101), groups).astype(jnp.int32)
    group_place = jnp.zeros((groups,), jnp.int32).at[group_order].set(jnp.arange(groups, dtype=jnp.int32))
    is_heavy = group_place < half_count
    partner = group_order[(group_place + half_count) % groups]
    long_len = jax.random.randint(jax.random.fold_in(key, 102), (groups, 2), 3 * DRAFT // 4, DRAFT + 1, jnp.int32)
    short_len = jax.random.randint(jax.random.fold_in(key, 103), (groups, 2), 8, DRAFT // 4 + 1, jnp.int32)
    lengths = jnp.where(is_heavy[:, None], long_len, short_len)
    lengths = lengths.at[group_order[0], 1].set(DRAFT)
    lengths = lengths.at[group_order[half_count]].set(DRAFT // 4)
    own_group = jnp.arange(groups, dtype=jnp.int32)
    dest = jnp.stack([own_group, jnp.where(is_heavy, partner, own_group)], axis=1)
    light_load = lengths[:, 0] + lengths[:, 1]
    offset = jnp.stack([jnp.zeros((groups,), jnp.int32), jnp.where(is_heavy, light_load[partner], lengths[:, 0])], axis=1)
    return (lengths.reshape(-1).astype(jnp.int32), dest.reshape(-1).astype(jnp.int32), offset.reshape(-1).astype(jnp.int32))


def draw_draft_lengths(key, part):
    return plan_tables(key)[0]


def draw_dest_group(key, part):
    return plan_tables(key)[1]


def draw_dest_offset(key, part):
    return plan_tables(key)[2]


def plant(result, own_key, low, largest):
    shape = result.shape
    index_at = [jax.random.randint(jax.random.fold_in(own_key, axis), (), 0, shape[axis]) for axis in range(len(shape))]
    result = result.at[tuple(index_at)].set(low)
    longest = shape.index(max(shape))
    index_at[longest] = (index_at[longest] + 1) % shape[longest]
    return result.at[tuple(index_at)].set(largest)


def levels(own_key, shape, pieces, low, top_value):
    factor_of, own = 1.0, jax.random.fold_in(own_key, 6)
    for axis_at, blocks in pieces:
        steps = jnp.exp(jax.random.uniform(jax.random.fold_in(own, axis_at), (blocks,), jnp.float32, low / len(pieces), top_value / len(pieces)))
        factor_of = factor_of * jnp.repeat(steps, shape[axis_at] // blocks).reshape([-1 if axis == axis_at else 1 for axis in range(len(shape))])
    return factor_of


def bell_draw(stream_key, extent, spread, reach, pieces=(), kind=jnp.bfloat16):
    entries = spread * jax.random.normal(stream_key, extent, jnp.float32)
    if pieces:
        entries = entries * levels(stream_key, extent, pieces, -0.22, 0.18)
    return jnp.clip(entries, -reach, reach).astype(kind)


def setup_inputs(seed: int = 0) -> dict:
    arg_keys = jax.random.split(jax.random.key(seed), 11)
    return {
        "queries": draw_queries(jax.random.fold_in(arg_keys[10], 71), 0),
        "draft_keys": bell_draw(arg_keys[1], (TOKENS, KV_HEADS * HEAD_DIM), 1.0, 6.0, ((0, 32),)),
        "draft_values": bell_draw(arg_keys[2], (TOKENS, KV_HEADS * HEAD_DIM), 1.0, 6.0, ((0, 32),)),
        "cache_keys": draw_cache_keys(jax.random.fold_in(arg_keys[10], 71), 0),
        "cache_values": bell_draw(arg_keys[4], (REQUESTS, CACHE, KV_HEADS * HEAD_DIM), 1.0, 6.0, ((0, 32), (1, 16))),
        "out_weight": bell_draw(arg_keys[5], (HEADS * HEAD_DIM, MODEL_DIM), (HEADS * HEAD_DIM // 32) ** -0.5, 0.25, ((0, 16), (1, 32))),
        "cache_lengths": plant(jax.random.randint(arg_keys[6], (REQUESTS,), CACHE // 4, CACHE + 1), jax.random.fold_in(arg_keys[6], 1), CACHE // 4, CACHE).astype(jnp.int32),
        "draft_lengths": draw_draft_lengths(jax.random.fold_in(arg_keys[10], 71), 0),
        "dest_group": draw_dest_group(jax.random.fold_in(arg_keys[10], 71), 0),
        "dest_offset": draw_dest_offset(jax.random.fold_in(arg_keys[10], 71), 0),
    }


NEG_FILL = -1e30


def packed_sources(row_ids, draft_lengths, dest_group, dest_offset):
    request_ids = jnp.arange(dest_group.shape[0], dtype=jnp.int32)
    slot_group = row_ids // PACK
    slot_index = row_ids % PACK
    inside = (dest_group[None, :] == slot_group[:, None]) & (slot_index[:, None] >= dest_offset[None, :]) & (slot_index[:, None] < (dest_offset + draft_lengths)[None, :])
    request = jnp.sum(jnp.where(inside, request_ids[None, :], 0), axis=1).astype(jnp.int32)
    first_slot = jnp.sum(jnp.where(inside, dest_offset[None, :], 0), axis=1).astype(jnp.int32)
    return request, (slot_index - first_slot).astype(jnp.int32), jnp.any(inside, axis=1)


def attend_request(operands):
    queries_one, cache_k, cache_v, draft_k, draft_v, cache_len, draft_len = operands
    score_scale = HEAD_DIM ** -0.5
    cache_scores = jnp.einsum("qkgd,lkd->kgql", queries_one.astype(jnp.float32), cache_k.astype(jnp.float32)) * score_scale
    draft_scores = jnp.einsum("qkgd,jkd->kgqj", queries_one.astype(jnp.float32), draft_k.astype(jnp.float32)) * score_scale
    cache_pos = jnp.arange(cache_k.shape[0], dtype=jnp.int32)
    draft_pos = jnp.arange(draft_k.shape[0], dtype=jnp.int32)
    keep_cache = cache_pos < cache_len
    keep_draft = (draft_pos[None, :] <= draft_pos[:, None]) & (draft_pos[None, :] < draft_len)
    cache_scores = jnp.where(keep_cache, cache_scores, NEG_FILL)
    draft_scores = jnp.where(keep_draft, draft_scores, NEG_FILL)
    highest = jnp.maximum(jnp.max(cache_scores, axis=-1, keepdims=True), jnp.max(draft_scores, axis=-1, keepdims=True))
    cache_exp = jnp.exp(cache_scores - highest)
    draft_exp = jnp.exp(draft_scores - highest)
    denominator = jnp.sum(cache_exp, axis=-1, keepdims=True) + jnp.sum(draft_exp, axis=-1, keepdims=True)
    cache_weights = (cache_exp / denominator).astype(jnp.bfloat16)
    draft_weights = (draft_exp / denominator).astype(jnp.bfloat16)
    mixed = jnp.einsum("kgql,lkd->qkgd", cache_weights.astype(jnp.float32), cache_v.astype(jnp.float32))
    mixed = mixed + jnp.einsum("kgqj,jkd->qkgd", draft_weights.astype(jnp.float32), draft_v.astype(jnp.float32))
    is_live = draft_pos < draft_len
    return jnp.where(is_live[:, None, None, None], mixed, 0.0).astype(jnp.bfloat16)


def reference(queries, draft_keys, draft_values, cache_keys, cache_values, out_weight, cache_lengths, draft_lengths, dest_group, dest_offset):
    group_heads = HEADS // KV_HEADS
    query_blocks = queries.reshape(REQUESTS, DRAFT, KV_HEADS, group_heads, HEAD_DIM)
    cache_k = cache_keys.reshape(REQUESTS, CACHE, KV_HEADS, HEAD_DIM)
    cache_v = cache_values.reshape(REQUESTS, CACHE, KV_HEADS, HEAD_DIM)
    draft_k = draft_keys.reshape(REQUESTS, DRAFT, KV_HEADS, HEAD_DIM)
    draft_v = draft_values.reshape(REQUESTS, DRAFT, KV_HEADS, HEAD_DIM)
    attended = lax.map(attend_request, (query_blocks, cache_k, cache_v, draft_k, draft_v, cache_lengths, draft_lengths))
    attended_rows = attended.reshape(REQUESTS * DRAFT, HEADS * HEAD_DIM)
    row_ids = jnp.arange(ROWS, dtype=jnp.int32)
    request, within, is_live = packed_sources(row_ids, draft_lengths, dest_group, dest_offset)
    row_index = (request * DRAFT + within).astype(jnp.int32)
    packed = jnp.where(is_live[:, None], jnp.take(attended_rows, row_index, axis=0), jnp.zeros((), jnp.bfloat16))
    block_width = HEADS * HEAD_DIM // N_TENSOR

    def add_block(index, running):
        first_col = (index * block_width).astype(jnp.int32)
        columns = lax.dynamic_slice_in_dim(packed, first_col, block_width, 1)
        weight_rows = lax.dynamic_slice_in_dim(out_weight, first_col, block_width, 0)
        partial_value = jnp.dot(columns, weight_rows, preferred_element_type=jnp.float32).astype(jnp.bfloat16)
        partial_value = lax.optimization_barrier(partial_value)
        return running + partial_value.astype(jnp.float32)

    running = lax.fori_loop(0, N_TENSOR, add_block, jnp.zeros((ROWS, MODEL_DIM), jnp.float32))
    return running.astype(jnp.bfloat16)
```

```python
import jax
import jax.numpy as jnp
from jax import lax
from jax.experimental import pallas as pl
from jax.experimental.pallas import tpu as pltpu
from jax.sharding import Mesh, PartitionSpec as P

HEAD_DIM = 128
DRAFT = 64
PACK = 96
REQUESTS = 64
NX, NY, NZ = 4, 8, 8
NEG_FILL = -1e30
BF16 = jnp.bfloat16
F32 = jnp.float32
NT = (((1,), (1,)), ((), ()))

FIRST = (0, -1, 1, -2, 2)
LAST = (-3, 3, -4)


def shift(value, axis, size, step):
    return lax.ppermute(value, axis, [(i, (i + step) % size) for i in range(size)])


def kv_kernel(k_ref, v_ref, o_ref):
    for h in range(NZ):
        o_ref[h, 0, 0] = k_ref[0, :, h * HEAD_DIM : (h + 1) * HEAD_DIM]
        o_ref[h, 1, 0] = v_ref[0, :, h * HEAD_DIM : (h + 1) * HEAD_DIM]


def pack_kv(k, v):
    return pl.pallas_call(
        kv_kernel,
        grid=(2,),
        in_specs=[pl.BlockSpec((1, 128, 1024), lambda r: (r, 0, 0))] * 2,
        out_specs=pl.BlockSpec((NZ, 2, 1, 128, 128), lambda r: (0, 0, r, 0, 0)),
        out_shape=jax.ShapeDtypeStruct((NZ, 2, 2, 128, 128), BF16),
        name="pack_kv",
    )(k, v)


def weight_kernel(s_ref, w_ref, o_ref):
    core = s_ref[0]
    wt = w_ref[...].T
    for zz in range(NZ):
        for cc in range(2):
            o_ref[lax.rem(core + cc, 2), zz] = wt[(zz * 2 + cc) * 32 : (zz * 2 + cc + 1) * 32]


def split_weight(core, w):
    return pl.pallas_call(
        weight_kernel,
        in_specs=[
            pl.BlockSpec(memory_space=pltpu.SMEM),
            pl.BlockSpec(memory_space=pltpu.VMEM),
        ],
        out_specs=pl.BlockSpec(memory_space=pltpu.VMEM),
        out_shape=jax.ShapeDtypeStruct((2, NZ, 32, 1024), BF16),
        name="split_weight",
    )(core, w)


def attend_kernel(s_ref, q_ref, own_ref, oth_ref, dk_ref, dv_ref, o_ref):
    r = pl.program_id(0)
    core = s_ref[1]
    cache_len = s_ref[2 + r]
    draft_len = s_ref[4 + r]
    scale = HEAD_DIM ** (-0.5)
    k_own = own_ref[:, 0, 0].reshape(1024, HEAD_DIM)
    k_oth = oth_ref[:, 0, 0].reshape(1024, HEAD_DIM)
    v_own = own_ref[:, 1, 0].reshape(1024, HEAD_DIM)
    v_oth = oth_ref[:, 1, 0].reshape(1024, HEAD_DIM)
    dk = dk_ref[...]
    dv = dv_ref[...]
    col = lax.broadcasted_iota(jnp.int32, (1, 1024), 1)
    pos = (col // 128) * 256 + col % 128
    keep_own = pos + core * 128 < cache_len
    keep_oth = pos + (1 - core) * 128 < cache_len
    row = lax.broadcasted_iota(jnp.int32, (128, DRAFT), 0) % DRAFT
    slot = lax.broadcasted_iota(jnp.int32, (128, DRAFT), 1)
    keep_draft = (slot <= row) & (slot < draft_len)
    live = lax.broadcasted_iota(jnp.int32, (128, 1), 0) % DRAFT < draft_len
    for pair in range(4):
        a, b = 2 * pair * HEAD_DIM, (2 * pair + 1) * HEAD_DIM
        q = jnp.concatenate([q_ref[:, a : a + HEAD_DIM], q_ref[:, b : b + HEAD_DIM]], axis=0)
        s_own = lax.dot_general(q, k_own, NT, preferred_element_type=F32) * scale
        s_oth = lax.dot_general(q, k_oth, NT, preferred_element_type=F32) * scale
        s_dr = lax.dot_general(q, dk, NT, preferred_element_type=F32) * scale
        s_own = jnp.where(keep_own, s_own, NEG_FILL)
        s_oth = jnp.where(keep_oth, s_oth, NEG_FILL)
        s_dr = jnp.where(keep_draft, s_dr, NEG_FILL)
        high = jnp.maximum(
            jnp.max(jnp.maximum(s_own, s_oth), axis=1, keepdims=True),
            jnp.max(s_dr, axis=1, keepdims=True),
        )
        e_own = jnp.exp(s_own - high)
        e_oth = jnp.exp(s_oth - high)
        e_dr = jnp.exp(s_dr - high)
        total = jnp.sum(e_own + e_oth, axis=1, keepdims=True) + jnp.sum(
            e_dr, axis=1, keepdims=True
        )
        mixed = jnp.dot(e_own.astype(BF16), v_own, preferred_element_type=F32)
        mixed = mixed + jnp.dot(e_oth.astype(BF16), v_oth, preferred_element_type=F32)
        mixed = mixed + jnp.dot(e_dr.astype(BF16), dv, preferred_element_type=F32)
        mixed = jnp.where(live, mixed / total, 0.0).astype(BF16)
        o_ref[:, a : a + HEAD_DIM] = mixed[:DRAFT]
        o_ref[:, b : b + HEAD_DIM] = mixed[DRAFT:]


def attend(scalars, q, own, oth, dk, dv):
    half = pl.BlockSpec((NZ, 2, 1, 128, 128), lambda r, s: (0, 0, r, 0, 0))
    draft = pl.BlockSpec((DRAFT, HEAD_DIM), lambda r, s: (r, s[0]))
    rows = pl.BlockSpec((DRAFT, 1024), lambda r, s: (r, 0))
    return pl.pallas_call(
        attend_kernel,
        grid_spec=pltpu.PrefetchScalarGridSpec(
            num_scalar_prefetch=1,
            grid=(2,),
            in_specs=[rows, half, half, draft, draft],
            out_specs=rows,
        ),
        out_shape=jax.ShapeDtypeStruct((2 * DRAFT, 1024), BF16),
        name="attend",
    )(scalars, q, own, oth, dk, dv)


def project_kernel(count, s_ref, *refs):
    mine, theirs, weights, o_ref = refs[:count], refs[count : 2 * count], refs[2 * count : -1], refs[-1]
    x = s_ref[0]
    a = jnp.concatenate([ref[...] for ref in mine], axis=0)
    b = jnp.concatenate([ref[...] for ref in theirs], axis=0)
    for step, ref in zip((0, -1, 1, 2), weights):
        acc = lax.dot_general(ref[0].reshape(256, 1024), a, NT, preferred_element_type=F32)
        acc = acc + lax.dot_general(ref[1].reshape(256, 1024), b, NT, preferred_element_type=F32)
        o_ref[lax.rem(x + step + NX, NX)] = acc.astype(BF16).reshape(NZ, 32, count * 128)


def project(x, mine, theirs, weights):
    count = len(mine)
    vmem = pl.BlockSpec(memory_space=pltpu.VMEM)
    return pl.pallas_call(
        lambda *refs: project_kernel(count, *refs),
        in_specs=[pl.BlockSpec(memory_space=pltpu.SMEM)] + [vmem] * (2 * count + NX),
        out_specs=vmem,
        out_shape=jax.ShapeDtypeStruct((NX, NZ, 32, count * 128), BF16),
        name="project",
    )(x, *mine, *theirs, *weights)


def place_kernel(s_ref, p_ref, q_ref, o_ref, f_ref):
    f_ref[...] = jnp.zeros(f_ref.shape, F32)
    my_y = s_ref[3 * REQUESTS]
    lane = lax.broadcasted_iota(jnp.int32, (32, 128), 1)
    for x in range(NX):
        for slots, ref in ((FIRST, p_ref), (LAST, q_ref)):
            for at, step in enumerate(slots):
                slab = ref[x, 0, :, at * 128 : (at + 1) * 128].astype(F32)
                for z in range(1, NZ):
                    slab = slab + ref[x, z, :, at * 128 : (at + 1) * 128].astype(F32)
                y = lax.rem(my_y + step + NY, NY)
                for r in range(2):
                    request = (x * NY + y) * 2 + r
                    length = s_ref[request]
                    group = s_ref[REQUESTS + request]
                    first = s_ref[2 * REQUESTS + request]
                    moved = pltpu.roll(slab, lax.rem(first + 64 * r, 128), 1)
                    keep = (lane >= first) & (lane < first + length)
                    f_ref[group] = f_ref[group] + jnp.where(keep, moved, 0.0)
    o_ref[...] = f_ref[...].astype(BF16)


def place(scalars, first, last):
    vmem = pl.BlockSpec(memory_space=pltpu.VMEM)
    return pl.pallas_call(
        place_kernel,
        in_specs=[pl.BlockSpec(memory_space=pltpu.SMEM), vmem, vmem],
        out_specs=vmem,
        out_shape=jax.ShapeDtypeStruct((32, 32, 128), BF16),
        scratch_shapes=[pltpu.VMEM((32, 32, 128), F32)],
        name="place",
    )(scalars, first, last)


def finish_kernel(i_ref, o_ref):
    for g in range(2):
        block = i_ref[:, g].reshape(512, 128).T
        o_ref[g * PACK : (g + 1) * PACK] = block[:PACK]


def finish(parts):
    vmem = pl.BlockSpec(memory_space=pltpu.VMEM)
    return pl.pallas_call(
        finish_kernel,
        in_specs=[vmem],
        out_specs=vmem,
        out_shape=jax.ShapeDtypeStruct((2 * PACK, 512), BF16),
        name="finish",
    )(parts)


def swap(value):
    return shift(value, "c", 2, 1)


def body(
    queries,
    draft_keys,
    draft_values,
    cache_keys,
    cache_values,
    out_weight,
    cache_lengths,
    draft_lengths,
    dest_group,
    dest_offset,
):
    x, y, z, c = (lax.axis_index(name).astype(jnp.int32) for name in ("x", "y", "z", "c"))
    my_lengths = lax.dynamic_slice_in_dim(draft_lengths, (x * NY + y) * 2, 2)
    heads = lax.all_to_all(pack_kv(cache_keys, cache_values), "z", 0, 0, tiled=True)

    halves = split_weight(c[None], out_weight)
    pair = jnp.stack([halves[0], swap(halves[1])])
    weights = [pair, shift(pair, "x", NX, 1), shift(pair, "x", NX, -1), shift(pair, "x", NX, 2)]

    others = swap(heads)
    scalars = jnp.concatenate([jnp.stack([z, c]), cache_lengths, my_lengths])
    rows = attend(scalars, queries, heads, others, draft_keys, draft_values)

    up1, down1 = shift(rows, "y", NY, 1), shift(rows, "y", NY, -1)
    up2, down2 = shift(rows, "y", NY, 2), shift(rows, "y", NY, -2)
    first = [rows, up1, down1, up2, down2]
    part1 = project(x[None], first, [swap(v) for v in first], weights)
    sums1 = lax.all_to_all(part1.reshape(32, 32, 640), ("x", "z"), 0, 0, tiled=True)
    up3, down3 = shift(up2, "y", NY, 1), shift(down2, "y", NY, -1)
    far = jnp.concatenate([shift(up2[:DRAFT], "y", NY, 2), shift(down2[DRAFT:], "y", NY, -2)])
    last = [up3, down3, far]
    part2 = project(x[None], last, [swap(v) for v in last], weights)
    sums2 = lax.all_to_all(part2.reshape(32, 32, 384), ("x", "z"), 0, 0, tiled=True)

    table = jnp.concatenate([draft_lengths, dest_group, dest_offset, y[None]])
    placed = place(table, sums1.reshape(NX, NZ, 32, 640), sums2.reshape(NX, NZ, 32, 384))
    parts = lax.all_to_all(placed.reshape(16, 2, 32, 128), ("z", "c"), 0, 0, tiled=True)
    return finish(parts)


def solution(mesh):
    fine = Mesh(mesh.devices.reshape(NX, NY, NZ, 2), ("x", "y", "z", "c"))
    xy, zc = ("x", "y"), ("z", "c")
    in_specs = (
        P(xy, zc),
        P(xy, None),
        P(xy, None),
        P(xy, zc, None),
        P(xy, zc, None),
        P(zc, xy),
        P(xy),
        P(),
        P(),
        P(),
    )
    return jax.shard_map(body, mesh=fine, in_specs=in_specs, out_specs=P(zc, xy), check_vma=False)
```

```python
import jax
import jax.numpy as jnp
from jax import lax
from jax.experimental import pallas as pl
from jax.experimental.pallas import tpu as pltpu
from jax.sharding import Mesh, PartitionSpec as P


HEAD_DIM = 128
DRAFT = 64
PACK = 96
REQUESTS = 64
NX, NY, NZ = 4, 8, 8
NEG_FILL = -1e30
BF16 = jnp.bfloat16
F32 = jnp.float32
NT = (((1,), (1,)), ((), ()))
VMEM = pl.BlockSpec(memory_space=pltpu.VMEM)
SMEM = pl.BlockSpec(memory_space=pltpu.SMEM)
ANY = pl.BlockSpec(memory_space=pl.ANY)
TOKEN = jax.ShapeDtypeStruct((8, 128), F32)

CHUNKS = ((0, -1, 1), (-2, 2), (-3, 3, -4))


def shift(value, axis, size, step):
    return lax.ppermute(value, axis, [(i, (i + step) % size) for i in range(size)])


def kv_kernel(k_ref, v_ref, o_ref):
    for h in range(NZ):
        o_ref[h, 0, 0] = k_ref[0, :, h * HEAD_DIM : (h + 1) * HEAD_DIM]
        o_ref[h, 0, 1] = v_ref[0, :, h * HEAD_DIM : (h + 1) * HEAD_DIM]


def pack_kv(k, v):
    return pl.pallas_call(
        kv_kernel,
        grid=(2,),
        in_specs=[pl.BlockSpec((1, 128, 1024), lambda r: (r, 0, 0))] * 2,
        out_specs=pl.BlockSpec((NZ, 1, 2, 128, 128), lambda r: (0, r, 0, 0, 0)),
        out_shape=jax.ShapeDtypeStruct((NZ, 2, 2, 128, 128), BF16),
        name="pack_kv",
    )(k, v)


def transpose_kernel(w_ref, o_ref):
    o_ref[...] = w_ref[...].T


def transpose(w):
    return pl.pallas_call(
        transpose_kernel,
        grid=(4,),
        in_specs=[pl.BlockSpec((1024, 128), lambda i: (0, i))],
        out_specs=pl.BlockSpec((128, 1024), lambda i: (i, 0)),
        out_shape=jax.ShapeDtypeStruct((512, 1024), BF16),
        name="transpose_w",
    )(w)


def attend_kernel(s_ref, mine_ref, other_ref, kv_ref, dk_ref, dv_ref, o_ref):
    cache_len = s_ref[2]
    draft_len = s_ref[3]
    scale = HEAD_DIM ** (-0.5)
    keys = kv_ref[:, 0].reshape(2048, HEAD_DIM)
    values = kv_ref[:, 1].reshape(2048, HEAD_DIM)
    dk = dk_ref[...]
    dv = dv_ref[...]
    keep = lax.broadcasted_iota(jnp.int32, (1, 2048), 1) < cache_len
    row = lax.broadcasted_iota(jnp.int32, (128, DRAFT), 0) % DRAFT
    slot = lax.broadcasted_iota(jnp.int32, (128, DRAFT), 1)
    keep_draft = (slot <= row) & (slot < draft_len)
    live = lax.broadcasted_iota(jnp.int32, (128, 1), 0) % DRAFT < draft_len
    for side, q_ref in enumerate((mine_ref, other_ref)):
        q = jnp.concatenate([q_ref[:, :HEAD_DIM], q_ref[:, HEAD_DIM:]], axis=0)
        cached = lax.dot_general(q, keys, NT, preferred_element_type=F32) * scale
        drafted = lax.dot_general(q, dk, NT, preferred_element_type=F32) * scale
        cached = jnp.where(keep, cached, NEG_FILL)
        drafted = jnp.where(keep_draft, drafted, NEG_FILL)
        high = jnp.maximum(
            jnp.max(cached, axis=1, keepdims=True), jnp.max(drafted, axis=1, keepdims=True)
        )
        cached = jnp.exp(cached - high)
        drafted = jnp.exp(drafted - high)
        total = jnp.sum(cached, axis=1, keepdims=True) + jnp.sum(drafted, axis=1, keepdims=True)
        mixed = jnp.dot(cached.astype(BF16), values, preferred_element_type=F32)
        mixed = mixed + jnp.dot(drafted.astype(BF16), dv, preferred_element_type=F32)
        mixed = jnp.where(live, mixed / total, 0.0).astype(BF16)
        o_ref[side, :, :HEAD_DIM] = mixed[:DRAFT]
        o_ref[side, :, HEAD_DIM:] = mixed[DRAFT:]


def attend(scalars, q, other_q, kv, dk, dv):
    draft = pl.BlockSpec((DRAFT, HEAD_DIM), lambda p, s: (s[1], s[0]))
    return pl.pallas_call(
        attend_kernel,
        grid_spec=pltpu.PrefetchScalarGridSpec(
            num_scalar_prefetch=1,
            grid=(4,),
            in_specs=[
                pl.BlockSpec((DRAFT, 256), lambda p, s: (s[1], p)),
                pl.BlockSpec((DRAFT, 256), lambda p, s: (0, p)),
                pl.BlockSpec((16, 2, 128, 128), lambda p, s: (0, 0, 0, 0)),
                draft,
                draft,
            ],
            out_specs=pl.BlockSpec((2, DRAFT, 256), lambda p, s: (0, 0, p)),
        ),
        out_shape=jax.ShapeDtypeStruct((2, DRAFT, 1024), BF16),
        name="attend",
    )(scalars, q, other_q, kv, dk, dv)


def project_kernel(count, s_ref, *refs):
    rows, own, far = refs[:count], refs[count : count + 4], refs[count + 4 : count + 8]
    o_ref, token_ref = refs[-2:]
    token_ref[...] = jnp.zeros(token_ref.shape, F32)
    x = s_ref[0]
    width = count * DRAFT
    a = jnp.concatenate([ref[0] for ref in rows], axis=0)
    b = jnp.concatenate([ref[1] for ref in rows], axis=0)
    for step, own_ref, far_ref in zip((0, -1, 1, 2), own, far):
        acc = lax.dot_general(own_ref[...], a, NT, preferred_element_type=F32)
        acc = acc + lax.dot_general(far_ref[...], b, NT, preferred_element_type=F32)
        acc = acc.astype(BF16).reshape(NZ, 2, 32, width)
        at = lax.rem(x + step + NX, NX)
        for half in range(2):
            o_ref[at, :, :, half * width : (half + 1) * width] = acc[:, half]


def project(x, rows, own, far, token):
    count = len(rows)
    return pl.pallas_call(
        lambda *refs: project_kernel(count, *refs),
        in_specs=[SMEM] + [VMEM] * (count + 8) + [ANY],
        out_specs=[VMEM, VMEM],
        out_shape=[jax.ShapeDtypeStruct((NX, NZ, 32, 2 * count * DRAFT), BF16), TOKEN],
        name="project",
    )(x, *rows, *own, *far, token)


def place_kernel(s_ref, *refs):
    parts, o_ref, f_ref = refs[:-2], refs[-2], refs[-1]
    f_ref[...] = jnp.zeros(f_ref.shape, F32)
    my_y = s_ref[3 * REQUESTS]
    core = s_ref[3 * REQUESTS + 1]
    lane = lax.broadcasted_iota(jnp.int32, (32, 128), 1)
    for x in range(NX):
        for slots, ref in zip(CHUNKS, parts):
            width = len(slots) * DRAFT
            for tile in range(2 * width // 128):
                slab = ref[x, 0, :, tile * 128 : (tile + 1) * 128].astype(F32)
                for z in range(1, NZ):
                    slab = slab + ref[x, z, :, tile * 128 : (tile + 1) * 128].astype(F32)
                for part in range(2):
                    column, at = divmod(2 * tile + part, len(slots))
                    request = (x * NY + lax.rem(my_y + slots[at] + NY, NY)) * 2 + core
                    length = s_ref[request]
                    group = s_ref[REQUESTS + request]
                    first = s_ref[2 * REQUESTS + request]
                    moved = pltpu.roll(slab, lax.rem(first + 64 * part, 128), 1)
                    keep = (lane >= first) & (lane < first + length)
                    spot = 2 * group + column
                    f_ref[spot] = f_ref[spot] + jnp.where(keep, moved, 0.0)
    for t in range(16):
        a, b, c, d = (f_ref[4 * t + i] for i in range(4))
        b, c, d = pltpu.roll(b, 96, 1), pltpu.roll(c, 64, 1), pltpu.roll(d, 32, 1)
        o_ref[t, :, :128] = jnp.where(lane < 96, a, b).astype(BF16)
        o_ref[t, :, 128:256] = jnp.where(lane < 64, b, c).astype(BF16)
        o_ref[t, :, 256:] = jnp.where(lane < 32, c, d).astype(BF16)


def place(scalars, parts):
    return pl.pallas_call(
        place_kernel,
        in_specs=[SMEM] + [VMEM] * len(parts),
        out_specs=VMEM,
        out_shape=jax.ShapeDtypeStruct((16, 32, 4 * PACK), BF16),
        scratch_shapes=[pltpu.VMEM((64, 32, 128), F32)],
        name="place",
    )(scalars, *parts)


def finish_kernel(i_ref, o_ref):
    lane = lax.broadcasted_iota(jnp.int32, (32, 128), 1)
    blocks = [[], []]
    for z in range(NZ):
        v = i_ref[2 * z].astype(F32) + i_ref[2 * z + 1].astype(F32)
        v = [v[:, i * 128 : (i + 1) * 128] for i in range(3)]
        blocks[0].append(v[0])
        blocks[0].append(pltpu.roll(jnp.where(lane < 64, v[1], v[0]), 32, 1))
        blocks[1].append(pltpu.roll(jnp.where(lane < 32, v[2], v[1]), 64, 1))
        blocks[1].append(pltpu.roll(v[2], 96, 1))
    for g in range(2):
        block = jnp.concatenate(blocks[g], axis=0).astype(BF16).T
        o_ref[g * PACK : (g + 1) * PACK] = block[:PACK]


def finish(parts):
    return pl.pallas_call(
        finish_kernel,
        in_specs=[VMEM],
        out_specs=VMEM,
        out_shape=jax.ShapeDtypeStruct((2 * PACK, 512), BF16),
        name="finish",
    )(parts)


def exchange(value, axes):
    return lax.all_to_all(value, axes, 0, 0, tiled=True)


def layer(
    queries,
    draft_keys,
    draft_values,
    cache_keys,
    cache_values,
    out_weight,
    cache_lengths,
    draft_lengths,
    dest_group,
    dest_offset,
):
    x, y, z, c = (lax.axis_index(name).astype(jnp.int32) for name in ("x", "y", "z", "c"))
    request = (x * NY + y) * 2 + c
    cache_length = lax.dynamic_slice_in_dim(cache_lengths, c, 1)
    draft_length = lax.dynamic_slice_in_dim(draft_lengths, request, 1)
    scalars = jnp.concatenate([jnp.stack([z, c]), cache_length, draft_length])
    table = jnp.concatenate([draft_lengths, dest_group, dest_offset, jnp.stack([y, c])])

    kv = exchange(pack_kv(cache_keys, cache_values).reshape(16, 2, 128, 128), ("z", "c"))

    w0 = transpose(out_weight)
    w1, w2 = shift(w0, "x", NX, 1), shift(w0, "x", NX, -1)
    w3 = jnp.concatenate([shift(w1[:256], "x", NX, 1), shift(w2[256:], "x", NX, -1)], axis=0)
    own = [w0, w1, w2, w3]
    far = [shift(w, "c", 2, 1) for w in own]
    other_q = lax.dynamic_slice_in_dim(queries, (1 - c) * DRAFT, DRAFT, 0)
    other_q = shift(other_q, "c", 2, 1)

    rows = attend(scalars, queries, other_q, kv, draft_keys, draft_values)
    up1, down1 = shift(rows, "y", NY, 1), shift(rows, "y", NY, -1)
    up2, down2 = shift(rows, "y", NY, 2), shift(rows, "y", NY, -2)
    up3, down3 = shift(up2, "y", NY, 1), shift(down2, "y", NY, -1)
    up4, down4 = shift(up2[:1], "y", NY, 2), shift(down2[1:], "y", NY, -2)
    arrived = {0: rows, -1: up1, 1: down1, -2: up2, 2: down2, -3: up3, 3: down3}
    arrived[-4] = jnp.concatenate([up4, down4], axis=0)

    token = jnp.zeros(TOKEN.shape, F32)
    sums = []
    for slots in CHUNKS:
        part, token = project(x[None], [arrived[s] for s in slots], own, far, token)
        part = part.reshape(NX * NZ, 32, -1)
        sums.append(exchange(part, ("x", "z")).reshape(NX, NZ, 32, -1))
    return finish(exchange(place(table, sums), ("z", "c")))


def solution(mesh):
    fine = Mesh(mesh.devices.reshape(NX, NY, NZ, 2), ("x", "y", "z", "c"))
    xy, zc = ("x", "y"), ("z", "c")
    in_specs = (
        P(xy, zc),
        P(xy, None),
        P(xy, None),
        P(xy, zc, None),
        P(xy, zc, None),
        P(zc, xy),
        P(xy),
        P(),
        P(),
        P(),
    )
    return jax.shard_map(layer, mesh=fine, in_specs=in_specs, out_specs=P(zc, xy), check_vma=False)
```

```python
import jax
import jax.numpy as jnp
from jax import lax
from jax.experimental import pallas as pl
from jax.experimental.pallas import tpu as pltpu
from jax.sharding import Mesh, PartitionSpec as P


HEAD_DIM = 128
DRAFT = 64
PACK = 96
NX, NY, NZ = 4, 8, 8
NEG_FILL = -1e30
BF16 = jnp.bfloat16
F32 = jnp.float32
NT = (((1,), (1,)), ((), ()))
VMEM = pl.BlockSpec(memory_space=pltpu.VMEM)
SMEM = pl.BlockSpec(memory_space=pltpu.SMEM)
ANY = pl.BlockSpec(memory_space=pl.ANY)
TOKEN = jax.ShapeDtypeStruct((8, 128), F32)

CHUNKS = ((0, -1, 1, -2), (2, -3, 3, -4))


def shift(value, axis, size, step):
    return lax.ppermute(value, axis, [(i, (i + step) % size) for i in range(size)])


def shift_cores(value, axis, size, step):
    pairs = [(2 * i + c, 2 * ((i + step * (1 - 2 * c)) % size) + c) for i in range(size) for c in (0, 1)]
    return lax.ppermute(value, (axis, "c"), pairs)


def kv_kernel(k_ref, v_ref, o_ref):
    for h in range(NZ):
        o_ref[h, 0, 0] = k_ref[0, :, h * HEAD_DIM : (h + 1) * HEAD_DIM]
        o_ref[h, 0, 1] = v_ref[0, :, h * HEAD_DIM : (h + 1) * HEAD_DIM]


def pack_kv(k, v):
    return pl.pallas_call(
        kv_kernel,
        grid=(2,),
        in_specs=[pl.BlockSpec((1, 128, 1024), lambda r: (r, 0, 0))] * 2,
        out_specs=pl.BlockSpec((NZ, 1, 2, 128, 128), lambda r: (0, r, 0, 0, 0)),
        out_shape=jax.ShapeDtypeStruct((NZ, 2, 2, 128, 128), BF16),
        name="pack_kv",
    )(k, v)


def transpose_kernel(w_ref, o_ref):
    o_ref[...] = w_ref[...].T


def transpose(w):
    return pl.pallas_call(
        transpose_kernel,
        grid=(4,),
        in_specs=[pl.BlockSpec((1024, 128), lambda i: (0, i))],
        out_specs=pl.BlockSpec((128, 1024), lambda i: (i, 0)),
        out_shape=jax.ShapeDtypeStruct((512, 1024), BF16),
        name="transpose_w",
    )(w)


def attend_kernel(s_ref, cache_ref, draft_ref, mine_ref, other_ref, kv_ref, dk_ref, dv_ref, o_ref):
    cache_len = cache_ref[s_ref[3]]
    draft_len = draft_ref[(s_ref[0] * NY + s_ref[1]) * 2 + s_ref[3]]
    scale = HEAD_DIM ** (-0.5)
    keys = kv_ref[:, 0].reshape(2048, HEAD_DIM)
    values = kv_ref[:, 1].reshape(2048, HEAD_DIM)
    dk = dk_ref[...]
    dv = dv_ref[...]
    keep = lax.broadcasted_iota(jnp.int32, (1, 2048), 1) < cache_len
    row = lax.broadcasted_iota(jnp.int32, (128, DRAFT), 0) % DRAFT
    slot = lax.broadcasted_iota(jnp.int32, (128, DRAFT), 1)
    keep_draft = (slot <= row) & (slot < draft_len)
    live = lax.broadcasted_iota(jnp.int32, (128, 1), 0) % DRAFT < draft_len
    for side, q_ref in enumerate((mine_ref, other_ref)):
        q = jnp.concatenate([q_ref[:, :HEAD_DIM], q_ref[:, HEAD_DIM:]], axis=0)
        cached = lax.dot_general(q, keys, NT, preferred_element_type=F32) * scale
        drafted = lax.dot_general(q, dk, NT, preferred_element_type=F32) * scale
        cached = jnp.where(keep, cached, NEG_FILL)
        drafted = jnp.where(keep_draft, drafted, NEG_FILL)
        high = jnp.maximum(
            jnp.max(cached, axis=1, keepdims=True), jnp.max(drafted, axis=1, keepdims=True)
        )
        cached = jnp.exp(cached - high)
        drafted = jnp.exp(drafted - high)
        total = jnp.sum(cached, axis=1, keepdims=True) + jnp.sum(drafted, axis=1, keepdims=True)
        mixed = jnp.dot(cached.astype(BF16), values, preferred_element_type=F32)
        mixed = mixed + jnp.dot(drafted.astype(BF16), dv, preferred_element_type=F32)
        mixed = jnp.where(live, mixed / total, 0.0).astype(BF16)
        o_ref[side, :, :HEAD_DIM] = mixed[:DRAFT]
        o_ref[side, :, HEAD_DIM:] = mixed[DRAFT:]


def attend(ids, cache_lengths, draft_lengths, q, other_q, kv, dk, dv):
    draft = pl.BlockSpec((DRAFT, HEAD_DIM), lambda p, s, *_: (s[3], s[2]))
    return pl.pallas_call(
        attend_kernel,
        grid_spec=pltpu.PrefetchScalarGridSpec(
            num_scalar_prefetch=3,
            grid=(4,),
            in_specs=[
                pl.BlockSpec((DRAFT, 256), lambda p, s, *_: (s[3], p)),
                pl.BlockSpec((DRAFT, 256), lambda p, *_: (0, p)),
                pl.BlockSpec((16, 2, 128, 128), lambda p, *_: (0, 0, 0, 0)),
                draft,
                draft,
            ],
            out_specs=pl.BlockSpec((2, DRAFT, 256), lambda p, *_: (0, 0, p)),
        ),
        out_shape=jax.ShapeDtypeStruct((2, DRAFT, 1024), BF16),
        name="attend",
    )(ids, cache_lengths, draft_lengths, q, other_q, kv, dk, dv)


def project_kernel(count, s_ref, *refs):
    rows, weights = refs[:count], refs[count : count + 8]
    o_ref, token_ref, w_ref, sems = refs[-4:]
    copies = [pltpu.make_async_copy(w, w_ref.at[i], sems.at[i]) for i, w in enumerate(weights)]
    for copy in copies[:4]:
        copy.start()
    token_ref[...] = jnp.zeros(token_ref.shape, F32)
    width = count * DRAFT
    a = jnp.concatenate([ref[0] for ref in rows], axis=0)
    b = jnp.concatenate([ref[1] for ref in rows], axis=0)
    for i, step in enumerate((0, -1, 1, 2)):
        if i > 0 and 2 * i + 2 < 8:
            copies[2 * i + 2].start()
            copies[2 * i + 3].start()
        copies[2 * i].wait()
        copies[2 * i + 1].wait()
        acc = lax.dot_general(w_ref[2 * i], a, NT, preferred_element_type=F32)
        acc = acc + lax.dot_general(w_ref[2 * i + 1], b, NT, preferred_element_type=F32)
        acc = acc.astype(BF16).reshape(NZ, 2, 32, width)
        at = lax.rem(s_ref[0] + step + NX, NX)
        for half in range(2):
            o_ref[at, :, :, half * width : (half + 1) * width] = acc[:, half]


def project(ids, rows, weights, token):
    count = len(rows)
    return pl.pallas_call(
        lambda *refs: project_kernel(count, *refs),
        in_specs=[SMEM] + [VMEM] * count + [pl.BlockSpec(memory_space=pltpu.HBM)] * 8 + [ANY],
        out_specs=[VMEM, VMEM],
        out_shape=[jax.ShapeDtypeStruct((NX, NZ, 32, 2 * count * DRAFT), BF16), TOKEN],
        scratch_shapes=[pltpu.VMEM((8, 512, 1024), BF16), pltpu.SemaphoreType.DMA((8,))],
        name="project",
    )(ids, *rows, *weights, token)


def place_kernel(s_ref, length_ref, group_ref, first_ref, *refs):
    parts, o_ref, f_ref = refs[:-2], refs[-2], refs[-1]
    f_ref[...] = jnp.zeros(f_ref.shape, F32)
    my_y, core = s_ref[1], s_ref[3]
    lane = lax.broadcasted_iota(jnp.int32, (32, 128), 1)
    for x in range(NX):
        for slots, ref in zip(CHUNKS, parts):
            width = len(slots) * DRAFT
            for tile in range(2 * width // 128):
                slab = ref[x, 0, :, tile * 128 : (tile + 1) * 128].astype(F32)
                for z in range(1, NZ):
                    slab = slab + ref[x, z, :, tile * 128 : (tile + 1) * 128].astype(F32)
                for part in range(2):
                    column, at = divmod(2 * tile + part, len(slots))
                    request = (x * NY + lax.rem(my_y + slots[at] + NY, NY)) * 2 + core
                    length, group, first = length_ref[request], group_ref[request], first_ref[request]
                    moved = pltpu.roll(slab, lax.rem(first + 64 * part, 128), 1)
                    keep = (lane >= first) & (lane < first + length)
                    spot = 2 * group + column
                    f_ref[spot] = f_ref[spot] + jnp.where(keep, moved, 0.0)
    for t in range(16):
        a, b, c, d = (f_ref[4 * t + i] for i in range(4))
        b, c, d = pltpu.roll(b, 96, 1), pltpu.roll(c, 64, 1), pltpu.roll(d, 32, 1)
        o_ref[t, :, :128] = jnp.where(lane < 96, a, b).astype(BF16)
        o_ref[t, :, 128:256] = jnp.where(lane < 64, b, c).astype(BF16)
        o_ref[t, :, 256:] = jnp.where(lane < 32, c, d).astype(BF16)


def place(tables, parts):
    return pl.pallas_call(
        place_kernel,
        in_specs=[SMEM] * len(tables) + [VMEM] * len(parts),
        out_specs=VMEM,
        out_shape=jax.ShapeDtypeStruct((16, 32, 4 * PACK), BF16),
        scratch_shapes=[pltpu.VMEM((64, 32, 128), F32)],
        name="place",
    )(*tables, *parts)


def finish_kernel(i_ref, o_ref):
    lane = lax.broadcasted_iota(jnp.int32, (32, 128), 1)
    blocks = [[], []]
    for z in range(NZ):
        v = i_ref[2 * z].astype(F32) + i_ref[2 * z + 1].astype(F32)
        v = [v[:, i * 128 : (i + 1) * 128] for i in range(3)]
        blocks[0].append(v[0])
        blocks[0].append(pltpu.roll(jnp.where(lane < 64, v[1], v[0]), 32, 1))
        blocks[1].append(pltpu.roll(jnp.where(lane < 32, v[2], v[1]), 64, 1))
        blocks[1].append(pltpu.roll(v[2], 96, 1))
    for g in range(2):
        block = jnp.concatenate(blocks[g], axis=0).astype(BF16).T
        o_ref[g * PACK : (g + 1) * PACK] = block[:PACK]


def finish(parts):
    return pl.pallas_call(
        finish_kernel,
        in_specs=[VMEM],
        out_specs=VMEM,
        out_shape=jax.ShapeDtypeStruct((2 * PACK, 512), BF16),
        name="finish",
    )(parts)


def exchange(value, axes):
    return lax.all_to_all(value, axes, 0, 0, tiled=True)


def layer(
    queries,
    draft_keys,
    draft_values,
    cache_keys,
    cache_values,
    out_weight,
    cache_lengths,
    draft_lengths,
    dest_group,
    dest_offset,
):
    c = lax.axis_index("c")
    ids = jnp.stack([lax.axis_index(name) for name in ("x", "y", "z", "c")]).astype(jnp.int32)

    kv = exchange(pack_kv(cache_keys, cache_values).reshape(16, 2, 128, 128), ("z", "c"))

    w0 = transpose(out_weight)
    w1, w2 = shift(w0, "x", NX, 1), shift(w0, "x", NX, -1)
    w3 = shift_cores(jnp.where(c == 0, w1, w2), "x", NX, 1)
    weights = []
    for w in (w0, w1, w2, w3):
        weights += [w, shift(w, "c", 2, 1)]
    other_q = lax.dynamic_slice_in_dim(queries, (1 - c) * DRAFT, DRAFT, 0)
    other_q = shift(other_q, "c", 2, 1)

    rows = attend(ids, cache_lengths, draft_lengths, queries, other_q, kv, draft_keys, draft_values)
    up1, down1 = shift(rows, "y", NY, 1), shift(rows, "y", NY, -1)
    up2, down2 = shift(rows, "y", NY, 2), shift(rows, "y", NY, -2)
    up3, down3 = shift(up2, "y", NY, 1), shift(down2, "y", NY, -1)
    far = shift_cores(jnp.where(c == 0, up2, down2), "y", NY, 2)
    arrived = {0: rows, -1: up1, 1: down1, -2: up2, 2: down2, -3: up3, 3: down3, -4: far}

    token = jnp.zeros(TOKEN.shape, F32)
    sums = []
    for slots in CHUNKS:
        part, token = project(ids, [arrived[s] for s in slots], weights, token)
        part = part.reshape(NX * NZ, 32, -1)
        sums.append(exchange(part, ("x", "z")).reshape(NX, NZ, 32, -1))
    placed = place([ids, draft_lengths, dest_group, dest_offset], sums)
    return finish(exchange(placed, ("z", "c")))


def solution(mesh):
    fine = Mesh(mesh.devices.reshape(NX, NY, NZ, 2), ("x", "y", "z", "c"))
    xy, zc = ("x", "y"), ("z", "c")
    in_specs = (
        P(xy, zc),
        P(xy, None),
        P(xy, None),
        P(xy, zc, None),
        P(xy, zc, None),
        P(zc, xy),
        P(xy),
        P(),
        P(),
        P(),
    )
    return jax.shard_map(layer, mesh=fine, in_specs=in_specs, out_specs=P(zc, xy), check_vma=False)
```

```python
import jax
import jax.numpy as jnp
from jax import lax
from jax.experimental import pallas as pl
from jax.experimental.pallas import tpu as pltpu
from jax.sharding import Mesh, PartitionSpec as P


HEAD_DIM = 128
DRAFT = 64
PACK = 96
NX, NY, NZ = 4, 8, 8
NEG_FILL = -1e30
EXP2_SCALE = HEAD_DIM ** (-0.5) * 1.4426950408889634
BF16 = jnp.bfloat16
F32 = jnp.float32
NT = (((1,), (1,)), ((), ()))
VMEM = pl.BlockSpec(memory_space=pltpu.VMEM)
SMEM = pl.BlockSpec(memory_space=pltpu.SMEM)
ANY = pl.BlockSpec(memory_space=pl.ANY)
TOKEN = jax.ShapeDtypeStruct((8, 128), F32)

CHUNKS = ((0, -1, 1, -2), (2, -3, 3, -4))


def shift(value, axis, size, step):
    return lax.ppermute(value, axis, [(i, (i + step) % size) for i in range(size)])


def shift_cores(value, axis, size, step):
    pairs = [(2 * i + c, 2 * ((i + step * (1 - 2 * c)) % size) + c) for i in range(size) for c in (0, 1)]
    return lax.ppermute(value, (axis, "c"), pairs)


def kv_kernel(k_ref, v_ref, o_ref):
    for h in range(NZ):
        o_ref[h, 0, 0] = k_ref[0, :, h * HEAD_DIM : (h + 1) * HEAD_DIM]
        o_ref[h, 0, 1] = v_ref[0, :, h * HEAD_DIM : (h + 1) * HEAD_DIM]


def pack_kv(k, v):
    return pl.pallas_call(
        kv_kernel,
        grid=(2,),
        in_specs=[pl.BlockSpec((1, 128, 1024), lambda r: (r, 0, 0))] * 2,
        out_specs=pl.BlockSpec((NZ, 1, 2, 128, 128), lambda r: (0, r, 0, 0, 0)),
        out_shape=jax.ShapeDtypeStruct((NZ, 2, 2, 128, 128), BF16),
        name="pack_kv",
    )(k, v)


def attend_kernel(s_ref, cache_ref, draft_ref, mine_ref, other_ref, kv_ref, dk_ref, dv_ref, o_ref):
    cache_len = cache_ref[s_ref[3]]
    draft_len = draft_ref[(s_ref[0] * NY + s_ref[1]) * 2 + s_ref[3]]
    keys = kv_ref[:, 0].reshape(2048, HEAD_DIM)
    values = kv_ref[:, 1].reshape(2048, HEAD_DIM)
    dk = dk_ref[...]
    dv = dv_ref[...]
    keep = lax.broadcasted_iota(jnp.int32, (1, 2048), 1) < cache_len
    row = lax.broadcasted_iota(jnp.int32, (256, DRAFT), 0) % DRAFT
    slot = lax.broadcasted_iota(jnp.int32, (256, DRAFT), 1)
    keep_draft = (slot <= row) & (slot < draft_len)
    live = lax.broadcasted_iota(jnp.int32, (256, 1), 0) % DRAFT < draft_len
    for side, q_ref in enumerate((mine_ref, other_ref)):
        q = jnp.concatenate([q_ref[:, h * HEAD_DIM : (h + 1) * HEAD_DIM] for h in range(4)], axis=0)
        cached = lax.dot_general(q, keys, NT, preferred_element_type=F32)
        drafted = lax.dot_general(q, dk, NT, preferred_element_type=F32)
        cached = jnp.where(keep, cached, NEG_FILL)
        drafted = jnp.where(keep_draft, drafted, NEG_FILL)
        high = jnp.maximum(
            jnp.max(cached, axis=1, keepdims=True), jnp.max(drafted, axis=1, keepdims=True)
        )
        cached = jnp.exp2((cached - high) * EXP2_SCALE)
        drafted = jnp.exp2((drafted - high) * EXP2_SCALE)
        total = jnp.sum(cached, axis=1, keepdims=True) + jnp.sum(drafted, axis=1, keepdims=True)
        mixed = jnp.dot(cached.astype(BF16), values, preferred_element_type=F32)
        mixed = mixed + jnp.dot(drafted.astype(BF16), dv, preferred_element_type=F32)
        mixed = jnp.where(live, mixed / total, 0.0).astype(BF16)
        for h in range(4):
            o_ref[side, :, h * HEAD_DIM : (h + 1) * HEAD_DIM] = mixed[h * DRAFT : (h + 1) * DRAFT]


def attend(ids, cache_lengths, draft_lengths, q, other_q, kv, dk, dv):
    draft = pl.BlockSpec((DRAFT, HEAD_DIM), lambda p, s, *_: (s[3], s[2]))
    return pl.pallas_call(
        attend_kernel,
        grid_spec=pltpu.PrefetchScalarGridSpec(
            num_scalar_prefetch=3,
            grid=(2,),
            in_specs=[
                pl.BlockSpec((DRAFT, 512), lambda p, s, *_: (s[3], p)),
                pl.BlockSpec((DRAFT, 512), lambda p, *_: (0, p)),
                pl.BlockSpec((16, 2, 128, 128), lambda p, *_: (0, 0, 0, 0)),
                draft,
                draft,
            ],
            out_specs=pl.BlockSpec((2, DRAFT, 512), lambda p, *_: (0, 0, p)),
        ),
        out_shape=jax.ShapeDtypeStruct((2, DRAFT, 1024), BF16),
        name="attend",
    )(ids, cache_lengths, draft_lengths, q, other_q, kv, dk, dv)


def project_kernel(count, s_ref, *refs):
    rows, weights = refs[:count], refs[count : count + 8]
    o_ref, token_ref, w_ref, sems = refs[-4:]
    copies = [pltpu.make_async_copy(w, w_ref.at[i], sems.at[i]) for i, w in enumerate(weights)]
    for copy in copies[:4]:
        copy.start()
    token_ref[...] = jnp.zeros(token_ref.shape, F32)
    width = count * DRAFT
    a = jnp.concatenate([ref[0] for ref in rows], axis=0)
    b = jnp.concatenate([ref[1] for ref in rows], axis=0)
    for i, step in enumerate((0, -1, 1, 2)):
        if 0 < i < 3:
            copies[2 * i + 2].start()
            copies[2 * i + 3].start()
        copies[2 * i].wait()
        copies[2 * i + 1].wait()
        acc = jnp.dot(a, w_ref[2 * i], preferred_element_type=F32)
        acc = acc + jnp.dot(b, w_ref[2 * i + 1], preferred_element_type=F32)
        acc = acc.astype(BF16).T.reshape(NZ, 2, 32, width)
        at = lax.rem(s_ref[0] + step + NX, NX)
        for half in range(2):
            o_ref[at, :, :, half * width : (half + 1) * width] = acc[:, half]


def project(ids, rows, weights, token):
    count = len(rows)
    return pl.pallas_call(
        lambda *refs: project_kernel(count, *refs),
        in_specs=[SMEM] + [VMEM] * count + [pl.BlockSpec(memory_space=pltpu.HBM)] * 8 + [ANY],
        out_specs=[VMEM, VMEM],
        out_shape=[jax.ShapeDtypeStruct((NX, NZ, 32, 2 * count * DRAFT), BF16), TOKEN],
        scratch_shapes=[pltpu.VMEM((8, 1024, 512), BF16), pltpu.SemaphoreType.DMA((8,))],
        name="project",
    )(ids, *rows, *weights, token)


def place_kernel(s_ref, length_ref, group_ref, first_ref, *refs):
    parts, o_ref, f_ref = refs[:-2], refs[-2], refs[-1]
    f_ref[...] = jnp.zeros(f_ref.shape, F32)
    my_y, core = s_ref[1], s_ref[3]
    lane = lax.broadcasted_iota(jnp.int32, (32, 128), 1)
    for x in range(NX):
        for slots, ref in zip(CHUNKS, parts):
            width = len(slots) * DRAFT
            for tile in range(2 * width // 128):
                slab = ref[x, 0, :, tile * 128 : (tile + 1) * 128].astype(F32)
                for z in range(1, NZ):
                    slab = slab + ref[x, z, :, tile * 128 : (tile + 1) * 128].astype(F32)
                for part in range(2):
                    column, at = divmod(2 * tile + part, len(slots))
                    request = (x * NY + lax.rem(my_y + slots[at] + NY, NY)) * 2 + core
                    length, group, first = length_ref[request], group_ref[request], first_ref[request]
                    moved = pltpu.roll(slab, lax.rem(first + 64 * part, 128), 1)
                    keep = (lane >= first) & (lane < first + length)
                    spot = 2 * group + column
                    f_ref[spot] = f_ref[spot] + jnp.where(keep, moved, 0.0)
    for t in range(16):
        a, b, c, d = (f_ref[4 * t + i] for i in range(4))
        b, c, d = pltpu.roll(b, 96, 1), pltpu.roll(c, 64, 1), pltpu.roll(d, 32, 1)
        o_ref[t, :, :128] = jnp.where(lane < 96, a, b).astype(BF16)
        o_ref[t, :, 128:256] = jnp.where(lane < 64, b, c).astype(BF16)
        o_ref[t, :, 256:] = jnp.where(lane < 32, c, d).astype(BF16)


def place(tables, parts):
    return pl.pallas_call(
        place_kernel,
        in_specs=[SMEM] * len(tables) + [VMEM] * len(parts),
        out_specs=VMEM,
        out_shape=jax.ShapeDtypeStruct((16, 32, 4 * PACK), BF16),
        scratch_shapes=[pltpu.VMEM((64, 32, 128), F32)],
        name="place",
    )(*tables, *parts)


def finish_kernel(i_ref, o_ref):
    lane = lax.broadcasted_iota(jnp.int32, (32, 128), 1)
    blocks = [[], []]
    for z in range(NZ):
        v = i_ref[2 * z].astype(F32) + i_ref[2 * z + 1].astype(F32)
        v = [v[:, i * 128 : (i + 1) * 128] for i in range(3)]
        blocks[0].append(v[0])
        blocks[0].append(pltpu.roll(jnp.where(lane < 64, v[1], v[0]), 32, 1))
        blocks[1].append(pltpu.roll(jnp.where(lane < 32, v[2], v[1]), 64, 1))
        blocks[1].append(pltpu.roll(v[2], 96, 1))
    for g in range(2):
        block = jnp.concatenate(blocks[g], axis=0).astype(BF16).T
        o_ref[g * PACK : (g + 1) * PACK] = block[:PACK]


def finish(parts):
    return pl.pallas_call(
        finish_kernel,
        in_specs=[VMEM],
        out_specs=VMEM,
        out_shape=jax.ShapeDtypeStruct((2 * PACK, 512), BF16),
        name="finish",
    )(parts)


def exchange(value, axes):
    return lax.all_to_all(value, axes, 0, 0, tiled=True)


def layer(
    queries,
    draft_keys,
    draft_values,
    cache_keys,
    cache_values,
    out_weight,
    cache_lengths,
    draft_lengths,
    dest_group,
    dest_offset,
):
    c = lax.axis_index("c")
    ids = jnp.stack([lax.axis_index(name) for name in ("x", "y", "z", "c")]).astype(jnp.int32)

    kv = exchange(pack_kv(cache_keys, cache_values).reshape(16, 2, 128, 128), ("z", "c"))

    w1, w2 = shift(out_weight, "x", NX, 1), shift(out_weight, "x", NX, -1)
    w3 = shift_cores(jnp.where(c == 0, w1, w2), "x", NX, 1)
    weights = []
    for w in (out_weight, w1, w2, w3):
        weights += [w, shift(w, "c", 2, 1)]
    other_q = lax.dynamic_slice_in_dim(queries, (1 - c) * DRAFT, DRAFT, 0)
    other_q = shift(other_q, "c", 2, 1)

    rows = attend(ids, cache_lengths, draft_lengths, queries, other_q, kv, draft_keys, draft_values)
    up1, down1 = shift(rows, "y", NY, 1), shift(rows, "y", NY, -1)
    up2, down2 = shift(rows, "y", NY, 2), shift(rows, "y", NY, -2)
    up3, down3 = shift(up2, "y", NY, 1), shift(down2, "y", NY, -1)
    far = shift_cores(jnp.where(c == 0, up2, down2), "y", NY, 2)
    arrived = {0: rows, -1: up1, 1: down1, -2: up2, 2: down2, -3: up3, 3: down3, -4: far}

    token = jnp.zeros(TOKEN.shape, F32)
    sums = []
    for slots in CHUNKS:
        part, token = project(ids, [arrived[s] for s in slots], weights, token)
        part = part.reshape(NX * NZ, 32, -1)
        sums.append(exchange(part, ("x", "z")).reshape(NX, NZ, 32, -1))
    placed = place([ids, draft_lengths, dest_group, dest_offset], sums)
    return finish(exchange(placed, ("z", "c")))


def solution(mesh):
    fine = Mesh(mesh.devices.reshape(NX, NY, NZ, 2), ("x", "y", "z", "c"))
    xy, zc = ("x", "y"), ("z", "c")
    in_specs = (
        P(xy, zc),
        P(xy, None),
        P(xy, None),
        P(xy, zc, None),
        P(xy, zc, None),
        P(zc, xy),
        P(xy),
        P(),
        P(),
        P(),
    )
    return jax.shard_map(layer, mesh=fine, in_specs=in_specs, out_specs=P(zc, xy), check_vma=False)
```

```python
import jax
import jax.numpy as jnp
from jax import lax
from jax.experimental import pallas as pl
from jax.experimental.pallas import tpu as pltpu
from jax.sharding import Mesh, PartitionSpec as P


HEAD_DIM = 128
DRAFT = 64
PACK = 96
NX, NY, NZ = 4, 8, 8
NEG_FILL = -1e30
EXP2_SCALE = HEAD_DIM ** (-0.5) * 1.4426950408889634
BF16 = jnp.bfloat16
F32 = jnp.float32
NT = (((1,), (1,)), ((), ()))
VMEM = pl.BlockSpec(memory_space=pltpu.VMEM)
SMEM = pl.BlockSpec(memory_space=pltpu.SMEM)
ANY = pl.BlockSpec(memory_space=pl.ANY)
TOKEN = jax.ShapeDtypeStruct((8, 128), F32)

CHUNKS = ((0, -1, 1, -2, 2, -3, 3, -4),)


def shift(value, axis, size, step):
    return lax.ppermute(value, axis, [(i, (i + step) % size) for i in range(size)])


def shift_cores(value, axis, size, step):
    pairs = [(2 * i + c, 2 * ((i + step * (1 - 2 * c)) % size) + c) for i in range(size) for c in (0, 1)]
    return lax.ppermute(value, (axis, "c"), pairs)


def kv_kernel(k_ref, v_ref, o_ref):
    for h in range(NZ):
        o_ref[h, 0, 0] = k_ref[0, :, h * HEAD_DIM : (h + 1) * HEAD_DIM]
        o_ref[h, 0, 1] = v_ref[0, :, h * HEAD_DIM : (h + 1) * HEAD_DIM]


def pack_kv(k, v):
    return pl.pallas_call(
        kv_kernel,
        grid=(2,),
        in_specs=[pl.BlockSpec((1, 128, 1024), lambda r: (r, 0, 0))] * 2,
        out_specs=pl.BlockSpec((NZ, 1, 2, 128, 128), lambda r: (0, r, 0, 0, 0)),
        out_shape=jax.ShapeDtypeStruct((NZ, 2, 2, 128, 128), BF16),
        name="pack_kv",
    )(k, v)


def attend_kernel(s_ref, cache_ref, draft_ref, mine_ref, other_ref, kv_ref, dk_ref, dv_ref, o_ref):
    cache_len = cache_ref[s_ref[3]]
    draft_len = draft_ref[(s_ref[0] * NY + s_ref[1]) * 2 + s_ref[3]]
    keys = kv_ref[:, 0].reshape(2048, HEAD_DIM)
    values = kv_ref[:, 1].reshape(2048, HEAD_DIM)
    dk = dk_ref[...]
    dv = dv_ref[...]
    keep = lax.broadcasted_iota(jnp.int32, (1, 2048), 1) < cache_len
    row = lax.broadcasted_iota(jnp.int32, (256, DRAFT), 0) % DRAFT
    slot = lax.broadcasted_iota(jnp.int32, (256, DRAFT), 1)
    keep_draft = (slot <= row) & (slot < draft_len)
    live = lax.broadcasted_iota(jnp.int32, (256, 1), 0) % DRAFT < draft_len
    for side, q_ref in enumerate((mine_ref, other_ref)):
        q = jnp.concatenate([q_ref[:, h * HEAD_DIM : (h + 1) * HEAD_DIM] for h in range(4)], axis=0)
        cached = lax.dot_general(q, keys, NT, preferred_element_type=F32)
        drafted = lax.dot_general(q, dk, NT, preferred_element_type=F32)
        cached = jnp.where(keep, cached, NEG_FILL)
        drafted = jnp.where(keep_draft, drafted, NEG_FILL)
        high = jnp.maximum(
            jnp.max(cached, axis=1, keepdims=True), jnp.max(drafted, axis=1, keepdims=True)
        )
        cached = jnp.exp2((cached - high) * EXP2_SCALE)
        drafted = jnp.exp2((drafted - high) * EXP2_SCALE)
        total = jnp.sum(cached, axis=1, keepdims=True) + jnp.sum(drafted, axis=1, keepdims=True)
        mixed = jnp.dot(cached.astype(BF16), values, preferred_element_type=F32)
        mixed = mixed + jnp.dot(drafted.astype(BF16), dv, preferred_element_type=F32)
        mixed = jnp.where(live, mixed / total, 0.0).astype(BF16)
        for h in range(4):
            o_ref[side, :, h * HEAD_DIM : (h + 1) * HEAD_DIM] = mixed[h * DRAFT : (h + 1) * DRAFT]


def attend(ids, cache_lengths, draft_lengths, q, other_q, kv, dk, dv):
    draft = pl.BlockSpec((DRAFT, HEAD_DIM), lambda p, s, *_: (s[3], s[2]))
    return pl.pallas_call(
        attend_kernel,
        grid_spec=pltpu.PrefetchScalarGridSpec(
            num_scalar_prefetch=3,
            grid=(2,),
            in_specs=[
                pl.BlockSpec((DRAFT, 512), lambda p, s, *_: (s[3], p)),
                pl.BlockSpec((DRAFT, 512), lambda p, *_: (0, p)),
                pl.BlockSpec((16, 2, 128, 128), lambda p, *_: (0, 0, 0, 0)),
                draft,
                draft,
            ],
            out_specs=pl.BlockSpec((2, DRAFT, 512), lambda p, *_: (0, 0, p)),
        ),
        out_shape=jax.ShapeDtypeStruct((2, DRAFT, 1024), BF16),
        name="attend",
    )(ids, cache_lengths, draft_lengths, q, other_q, kv, dk, dv)


def project_kernel(count, s_ref, *refs):
    rows, weights = refs[:count], refs[count : count + 8]
    o_ref, token_ref, w_ref, sems = refs[-4:]
    copies = [pltpu.make_async_copy(w, w_ref.at[i], sems.at[i]) for i, w in enumerate(weights)]
    for copy in copies[:4]:
        copy.start()
    token_ref[...] = jnp.zeros(token_ref.shape, F32)
    width = count * DRAFT
    a = jnp.concatenate([ref[0] for ref in rows], axis=0)
    b = jnp.concatenate([ref[1] for ref in rows], axis=0)
    for i, step in enumerate((0, -1, 1, 2)):
        if 0 < i < 3:
            copies[2 * i + 2].start()
            copies[2 * i + 3].start()
        copies[2 * i].wait()
        copies[2 * i + 1].wait()
        acc = jnp.dot(a, w_ref[2 * i], preferred_element_type=F32)
        acc = acc + jnp.dot(b, w_ref[2 * i + 1], preferred_element_type=F32)
        acc = acc.astype(BF16).T.reshape(NZ, 2, 32, width)
        at = lax.rem(s_ref[0] + step + NX, NX)
        for half in range(2):
            o_ref[at, :, :, half * width : (half + 1) * width] = acc[:, half]


def project(ids, rows, weights, token):
    count = len(rows)
    return pl.pallas_call(
        lambda *refs: project_kernel(count, *refs),
        in_specs=[SMEM] + [VMEM] * count + [pl.BlockSpec(memory_space=pltpu.HBM)] * 8 + [ANY],
        out_specs=[VMEM, VMEM],
        out_shape=[jax.ShapeDtypeStruct((NX, NZ, 32, 2 * count * DRAFT), BF16), TOKEN],
        scratch_shapes=[pltpu.VMEM((8, 1024, 512), BF16), pltpu.SemaphoreType.DMA((8,))],
        name="project",
    )(ids, *rows, *weights, token)


def place_kernel(s_ref, length_ref, group_ref, first_ref, *refs):
    parts, o_ref, f_ref = refs[:-2], refs[-2], refs[-1]
    f_ref[...] = jnp.zeros(f_ref.shape, F32)
    my_y, core = s_ref[1], s_ref[3]
    lane = lax.broadcasted_iota(jnp.int32, (32, 128), 1)
    for x in range(NX):
        for slots, ref in zip(CHUNKS, parts):
            width = len(slots) * DRAFT
            for tile in range(2 * width // 128):
                slab = ref[x, 0, :, tile * 128 : (tile + 1) * 128].astype(F32)
                for z in range(1, NZ):
                    slab = slab + ref[x, z, :, tile * 128 : (tile + 1) * 128].astype(F32)
                for part in range(2):
                    column, at = divmod(2 * tile + part, len(slots))
                    request = (x * NY + lax.rem(my_y + slots[at] + NY, NY)) * 2 + core
                    length, group, first = length_ref[request], group_ref[request], first_ref[request]
                    moved = pltpu.roll(slab, lax.rem(first + 64 * part, 128), 1)
                    keep = (lane >= first) & (lane < first + length)
                    spot = 2 * group + column
                    f_ref[spot] = f_ref[spot] + jnp.where(keep, moved, 0.0)
    for t in range(16):
        a, b, c, d = (f_ref[4 * t + i] for i in range(4))
        b, c, d = pltpu.roll(b, 96, 1), pltpu.roll(c, 64, 1), pltpu.roll(d, 32, 1)
        o_ref[t, :, :128] = jnp.where(lane < 96, a, b).astype(BF16)
        o_ref[t, :, 128:256] = jnp.where(lane < 64, b, c).astype(BF16)
        o_ref[t, :, 256:] = jnp.where(lane < 32, c, d).astype(BF16)


def place(tables, parts):
    return pl.pallas_call(
        place_kernel,
        in_specs=[SMEM] * len(tables) + [VMEM] * len(parts),
        out_specs=VMEM,
        out_shape=jax.ShapeDtypeStruct((16, 32, 4 * PACK), BF16),
        scratch_shapes=[pltpu.VMEM((64, 32, 128), F32)],
        name="place",
    )(*tables, *parts)


def finish_kernel(i_ref, o_ref):
    lane = lax.broadcasted_iota(jnp.int32, (32, 128), 1)
    blocks = [[], []]
    for z in range(NZ):
        v = i_ref[2 * z].astype(F32) + i_ref[2 * z + 1].astype(F32)
        v = [v[:, i * 128 : (i + 1) * 128] for i in range(3)]
        blocks[0].append(v[0])
        blocks[0].append(pltpu.roll(jnp.where(lane < 64, v[1], v[0]), 32, 1))
        blocks[1].append(pltpu.roll(jnp.where(lane < 32, v[2], v[1]), 64, 1))
        blocks[1].append(pltpu.roll(v[2], 96, 1))
    for g in range(2):
        block = jnp.concatenate(blocks[g], axis=0).astype(BF16).T
        o_ref[g * PACK : (g + 1) * PACK] = block[:PACK]


def finish(parts):
    return pl.pallas_call(
        finish_kernel,
        in_specs=[VMEM],
        out_specs=VMEM,
        out_shape=jax.ShapeDtypeStruct((2 * PACK, 512), BF16),
        name="finish",
    )(parts)


def exchange(value, axes):
    return lax.all_to_all(value, axes, 0, 0, tiled=True)


def layer(
    queries,
    draft_keys,
    draft_values,
    cache_keys,
    cache_values,
    out_weight,
    cache_lengths,
    draft_lengths,
    dest_group,
    dest_offset,
):
    c = lax.axis_index("c")
    ids = jnp.stack([lax.axis_index(name) for name in ("x", "y", "z", "c")]).astype(jnp.int32)

    kv = exchange(pack_kv(cache_keys, cache_values).reshape(16, 2, 128, 128), ("z", "c"))

    w1, w2 = shift(out_weight, "x", NX, 1), shift(out_weight, "x", NX, -1)
    w3 = shift_cores(jnp.where(c == 0, w1, w2), "x", NX, 1)
    weights = []
    for w in (out_weight, w1, w2, w3):
        weights += [w, shift(w, "c", 2, 1)]
    other_q = lax.dynamic_slice_in_dim(queries, (1 - c) * DRAFT, DRAFT, 0)
    other_q = shift(other_q, "c", 2, 1)

    rows = attend(ids, cache_lengths, draft_lengths, queries, other_q, kv, draft_keys, draft_values)
    up1, down1 = shift(rows, "y", NY, 1), shift(rows, "y", NY, -1)
    up2, down2 = shift(up1, "y", NY, 1), shift(down1, "y", NY, -1)
    up3, down3 = shift(up2, "y", NY, 1), shift(down2, "y", NY, -1)
    far = shift_cores(jnp.where(c == 0, up3, down3), "y", NY, 1)
    arrived = {0: rows, -1: up1, 1: down1, -2: up2, 2: down2, -3: up3, 3: down3, -4: far}

    token = jnp.zeros(TOKEN.shape, F32)
    sums = []
    for slots in CHUNKS:
        part, token = project(ids, [arrived[s] for s in slots], weights, token)
        part = part.reshape(NX * NZ, 32, -1)
        sums.append(exchange(part, ("x", "z")).reshape(NX, NZ, 32, -1))
    placed = place([ids, draft_lengths, dest_group, dest_offset], sums)
    return finish(exchange(placed, ("z", "c")))


def solution(mesh):
    fine = Mesh(mesh.devices.reshape(NX, NY, NZ, 2), ("x", "y", "z", "c"))
    xy, zc = ("x", "y"), ("z", "c")
    in_specs = (
        P(xy, zc),
        P(xy, None),
        P(xy, None),
        P(xy, zc, None),
        P(xy, zc, None),
        P(zc, xy),
        P(xy),
        P(),
        P(),
        P(),
    )
    return jax.shard_map(layer, mesh=fine, in_specs=in_specs, out_specs=P(zc, xy), check_vma=False)
```

```python
import jax
import jax.numpy as jnp
from jax import lax
from jax.experimental import pallas as pl
from jax.experimental.pallas import tpu as pltpu
from jax.sharding import Mesh, PartitionSpec as P


HEAD_DIM = 128
DRAFT = 64
PACK = 96
NX, NY, NZ = 4, 8, 8
NEG_FILL = -1e30
EXP2_SCALE = HEAD_DIM ** (-0.5) * 1.4426950408889634
BF16 = jnp.bfloat16
F32 = jnp.float32
NT = (((1,), (1,)), ((), ()))
VMEM = pl.BlockSpec(memory_space=pltpu.VMEM)
SMEM = pl.BlockSpec(memory_space=pltpu.SMEM)
PARAMS = pltpu.CompilerParams(vmem_limit_bytes=24 * 2**20)

CHUNKS = ((0, -1, 1, -2, 2), (-3, 3, -4))


def shift(value, axis, size, step):
    return lax.ppermute(value, axis, [(i, (i + step) % size) for i in range(size)])


def shift_cores(value, axis, size, step):
    pairs = [(2 * i + c, 2 * ((i + step * (1 - 2 * c)) % size) + c) for i in range(size) for c in (0, 1)]
    return lax.ppermute(value, (axis, "c"), pairs)


def near(value):
    return pltpu.with_memory_space_constraint(value, pltpu.VMEM)


def kv_kernel(k_ref, v_ref, o_ref):
    for h in range(NZ):
        o_ref[h, 0, 0] = k_ref[0, :, h * HEAD_DIM : (h + 1) * HEAD_DIM]
        o_ref[h, 0, 1] = v_ref[0, :, h * HEAD_DIM : (h + 1) * HEAD_DIM]


def pack_kv(k, v):
    return pl.pallas_call(
        kv_kernel,
        grid=(2,),
        in_specs=[pl.BlockSpec((1, 128, 1024), lambda r: (r, 0, 0))] * 2,
        out_specs=pl.BlockSpec((NZ, 1, 2, 128, 128), lambda r: (0, r, 0, 0, 0)),
        out_shape=pltpu.VMEM((NZ, 2, 2, 128, 128), BF16),
        compiler_params=PARAMS,
        name="pack_kv",
    )(k, v)


def attend_kernel(s_ref, cache_ref, draft_ref, mine_ref, other_ref, kv_ref, dk_ref, dv_ref, o_ref):
    cache_len = cache_ref[s_ref[3]]
    draft_len = draft_ref[(s_ref[0] * NY + s_ref[1]) * 2 + s_ref[3]]
    keys = kv_ref[:, 0].reshape(2048, HEAD_DIM)
    values = kv_ref[:, 1].reshape(2048, HEAD_DIM)
    dk = dk_ref[...]
    dv = dv_ref[...]
    keep = lax.broadcasted_iota(jnp.int32, (1, 2048), 1) < cache_len
    row = lax.broadcasted_iota(jnp.int32, (256, DRAFT), 0) % DRAFT
    slot = lax.broadcasted_iota(jnp.int32, (256, DRAFT), 1)
    keep_draft = (slot <= row) & (slot < draft_len)
    live = lax.broadcasted_iota(jnp.int32, (256, 1), 0) % DRAFT < draft_len
    for side, q_ref in enumerate((mine_ref, other_ref)):
        q = jnp.concatenate([q_ref[:, h * HEAD_DIM : (h + 1) * HEAD_DIM] for h in range(4)], axis=0)
        cached = lax.dot_general(q, keys, NT, preferred_element_type=F32)
        drafted = lax.dot_general(q, dk, NT, preferred_element_type=F32)
        cached = jnp.where(keep, cached, NEG_FILL)
        drafted = jnp.where(keep_draft, drafted, NEG_FILL)
        high = jnp.maximum(
            jnp.max(cached, axis=1, keepdims=True), jnp.max(drafted, axis=1, keepdims=True)
        )
        cached = jnp.exp2((cached - high) * EXP2_SCALE)
        drafted = jnp.exp2((drafted - high) * EXP2_SCALE)
        total = jnp.sum(cached, axis=1, keepdims=True) + jnp.sum(drafted, axis=1, keepdims=True)
        mixed = jnp.dot(cached.astype(BF16), values, preferred_element_type=F32)
        mixed = mixed + jnp.dot(drafted.astype(BF16), dv, preferred_element_type=F32)
        mixed = jnp.where(live, mixed / total, 0.0).astype(BF16)
        for h in range(4):
            o_ref[side, :, h * HEAD_DIM : (h + 1) * HEAD_DIM] = mixed[h * DRAFT : (h + 1) * DRAFT]


def attend(ids, cache_lengths, draft_lengths, q, other_q, kv, dk, dv):
    draft = pl.BlockSpec((DRAFT, HEAD_DIM), lambda p, s, *_: (s[3], s[2]))
    return pl.pallas_call(
        attend_kernel,
        grid_spec=pltpu.PrefetchScalarGridSpec(
            num_scalar_prefetch=3,
            grid=(2,),
            in_specs=[
                pl.BlockSpec((DRAFT, 512), lambda p, s, *_: (s[3], p)),
                pl.BlockSpec((DRAFT, 512), lambda p, *_: (0, p)),
                pl.BlockSpec((16, 2, 128, 128), lambda p, *_: (0, 0, 0, 0)),
                draft,
                draft,
            ],
            out_specs=pl.BlockSpec((2, DRAFT, 512), lambda p, *_: (0, 0, p)),
        ),
        out_shape=pltpu.VMEM((2, DRAFT, 1024), BF16),
        compiler_params=PARAMS,
        name="attend",
    )(ids, cache_lengths, draft_lengths, q, other_q, kv, dk, dv)


def project_kernel(count, s_ref, *refs):
    rows, weights, o_ref = refs[:count], refs[count:-1], refs[-1]
    width = count * DRAFT
    a = jnp.concatenate([ref[0] for ref in rows], axis=0)
    b = jnp.concatenate([ref[1] for ref in rows], axis=0)
    for i, step in enumerate((0, -1, 1, 2)):
        acc = jnp.dot(a, weights[2 * i][...], preferred_element_type=F32)
        acc = acc + jnp.dot(b, weights[2 * i + 1][...], preferred_element_type=F32)
        acc = acc.astype(BF16).T.reshape(NZ, 2, 32, width)
        at = lax.rem(s_ref[0] + step + NX, NX)
        for half in range(2):
            o_ref[at, :, :, half * width : (half + 1) * width] = acc[:, half]


def project(ids, rows, weights):
    count = len(rows)
    return pl.pallas_call(
        lambda *refs: project_kernel(count, *refs),
        in_specs=[SMEM] + [VMEM] * (count + 8),
        out_specs=VMEM,
        out_shape=pltpu.VMEM((NX, NZ, 32, 2 * count * DRAFT), BF16),
        compiler_params=PARAMS,
        name="project",
    )(ids, *map(near, rows), *map(near, weights))


def place_kernel(s_ref, length_ref, group_ref, first_ref, *refs):
    parts, o_ref, f_ref = refs[:-2], refs[-2], refs[-1]
    f_ref[...] = jnp.zeros(f_ref.shape, F32)
    my_y, core = s_ref[1], s_ref[3]
    lane = lax.broadcasted_iota(jnp.int32, (32, 128), 1)
    for x in range(NX):
        for slots, ref in zip(CHUNKS, parts):
            width = len(slots) * DRAFT
            for tile in range(2 * width // 128):
                slab = ref[x, 0, :, tile * 128 : (tile + 1) * 128].astype(F32)
                for z in range(1, NZ):
                    slab = slab + ref[x, z, :, tile * 128 : (tile + 1) * 128].astype(F32)
                for part in range(2):
                    column, at = divmod(2 * tile + part, len(slots))
                    request = (x * NY + lax.rem(my_y + slots[at] + NY, NY)) * 2 + core
                    length, group, first = length_ref[request], group_ref[request], first_ref[request]
                    moved = pltpu.roll(slab, lax.rem(first + 64 * part, 128), 1)
                    keep = (lane >= first) & (lane < first + length)
                    spot = 2 * group + column
                    f_ref[spot] = f_ref[spot] + jnp.where(keep, moved, 0.0)
    for t in range(16):
        a, b, c, d = (f_ref[4 * t + i] for i in range(4))
        b, c, d = pltpu.roll(b, 96, 1), pltpu.roll(c, 64, 1), pltpu.roll(d, 32, 1)
        o_ref[t, :, :128] = jnp.where(lane < 96, a, b).astype(BF16)
        o_ref[t, :, 128:256] = jnp.where(lane < 64, b, c).astype(BF16)
        o_ref[t, :, 256:] = jnp.where(lane < 32, c, d).astype(BF16)


def place(tables, parts):
    return pl.pallas_call(
        place_kernel,
        in_specs=[SMEM] * len(tables) + [VMEM] * len(parts),
        out_specs=VMEM,
        out_shape=pltpu.VMEM((16, 32, 4 * PACK), BF16),
        scratch_shapes=[pltpu.VMEM((64, 32, 128), F32)],
        compiler_params=PARAMS,
        name="place",
    )(*tables, *map(near, parts))


def finish_kernel(i_ref, o_ref):
    lane = lax.broadcasted_iota(jnp.int32, (32, 128), 1)
    blocks = [[], []]
    for z in range(NZ):
        v = i_ref[2 * z].astype(F32) + i_ref[2 * z + 1].astype(F32)
        v = [v[:, i * 128 : (i + 1) * 128] for i in range(3)]
        blocks[0].append(v[0])
        blocks[0].append(pltpu.roll(jnp.where(lane < 64, v[1], v[0]), 32, 1))
        blocks[1].append(pltpu.roll(jnp.where(lane < 32, v[2], v[1]), 64, 1))
        blocks[1].append(pltpu.roll(v[2], 96, 1))
    for g in range(2):
        block = jnp.concatenate(blocks[g], axis=0).astype(BF16).T
        o_ref[g * PACK : (g + 1) * PACK] = block[:PACK]


def finish(parts):
    return pl.pallas_call(
        finish_kernel,
        in_specs=[VMEM],
        out_specs=VMEM,
        out_shape=jax.ShapeDtypeStruct((2 * PACK, 512), BF16),
        compiler_params=PARAMS,
        name="finish",
    )(near(parts))


def exchange(value, axes):
    return lax.all_to_all(value, axes, 0, 0, tiled=True)


def layer(
    queries,
    draft_keys,
    draft_values,
    cache_keys,
    cache_values,
    out_weight,
    cache_lengths,
    draft_lengths,
    dest_group,
    dest_offset,
):
    c = lax.axis_index("c")
    ids = jnp.stack([lax.axis_index(name) for name in ("x", "y", "z", "c")]).astype(jnp.int32)

    kv = exchange(pack_kv(cache_keys, cache_values).reshape(16, 2, 128, 128), ("z", "c"))

    w1, w2 = shift(out_weight, "x", NX, 1), shift(out_weight, "x", NX, -1)
    w3 = shift_cores(out_weight, "x", NX, 2)
    weights = []
    for w in (out_weight, w1, w2, w3):
        weights += [w, shift(w, "c", 2, 1)]
    other_q = lax.dynamic_slice_in_dim(queries, (1 - c) * DRAFT, DRAFT, 0)
    other_q = shift(other_q, "c", 2, 1)

    rows = attend(ids, cache_lengths, draft_lengths, queries, other_q, kv, draft_keys, draft_values)
    up1, down1 = shift(rows, "y", NY, 1), shift(rows, "y", NY, -1)
    up2, down2 = shift(up1, "y", NY, 1), shift(down1, "y", NY, -1)
    up3, down3 = shift(up2, "y", NY, 1), shift(down2, "y", NY, -1)
    far = shift_cores(jnp.where(c == 0, up3, down3), "y", NY, 1)
    arrived = {0: rows, -1: up1, 1: down1, -2: up2, 2: down2, -3: up3, 3: down3, -4: far}

    sums = []
    for slots in CHUNKS:
        part = project(ids, [arrived[s] for s in slots], weights)
        part = part.reshape(NX * NZ, 32, -1)
        sums.append(exchange(part, ("x", "z")).reshape(NX, NZ, 32, -1))
    placed = place([ids, draft_lengths, dest_group, dest_offset], sums)
    return finish(exchange(placed, ("z", "c")))


def solution(mesh):
    fine = Mesh(mesh.devices.reshape(NX, NY, NZ, 2), ("x", "y", "z", "c"))
    xy, zc = ("x", "y"), ("z", "c")
    in_specs = (
        P(xy, zc),
        P(xy, None),
        P(xy, None),
        P(xy, zc, None),
        P(xy, zc, None),
        P(zc, xy),
        P(xy),
        P(),
        P(),
        P(),
    )
    return jax.shard_map(layer, mesh=fine, in_specs=in_specs, out_specs=P(zc, xy), check_vma=False)
```

```python
import jax
import jax.numpy as jnp
from jax import lax
from jax.experimental import pallas as pl
from jax.experimental.pallas import tpu as pltpu
from jax.sharding import Mesh, PartitionSpec as P


HEAD_DIM = 128
DRAFT = 64
PACK = 96
NX, NY, NZ = 4, 8, 8
NEG_FILL = -1e30
EXP2_SCALE = HEAD_DIM ** (-0.5) * 1.4426950408889634
BF16 = jnp.bfloat16
F32 = jnp.float32
NT = (((1,), (1,)), ((), ()))
VMEM = pl.BlockSpec(memory_space=pltpu.VMEM)
SMEM = pl.BlockSpec(memory_space=pltpu.SMEM)
PARAMS = pltpu.CompilerParams(vmem_limit_bytes=24 * 2**20)

CHUNKS = ((0, -1, 1, -2, 2), (-3, 3, -4))


def shift(value, axis, size, step):
    return lax.ppermute(value, axis, [(i, (i + step) % size) for i in range(size)])


def shift_cores(value, axis, size, step):
    pairs = [(2 * i + c, 2 * ((i + step * (1 - 2 * c)) % size) + c) for i in range(size) for c in (0, 1)]
    return lax.ppermute(value, (axis, "c"), pairs)


def near(value):
    return pltpu.with_memory_space_constraint(value, pltpu.VMEM)


def far_off(value):
    return pltpu.with_memory_space_constraint(value, pltpu.HBM)


def kv_kernel(k_ref, v_ref, o_ref):
    for h in range(NZ):
        o_ref[h, 0, 0] = k_ref[0, :, h * HEAD_DIM : (h + 1) * HEAD_DIM]
        o_ref[h, 0, 1] = v_ref[0, :, h * HEAD_DIM : (h + 1) * HEAD_DIM]


def pack_kv(k, v):
    return pl.pallas_call(
        kv_kernel,
        grid=(2,),
        in_specs=[pl.BlockSpec((1, 128, 1024), lambda r: (r, 0, 0))] * 2,
        out_specs=pl.BlockSpec((NZ, 1, 2, 128, 128), lambda r: (0, r, 0, 0, 0)),
        out_shape=pltpu.VMEM((NZ, 2, 2, 128, 128), BF16),
        compiler_params=PARAMS,
        name="pack_kv",
    )(far_off(k), far_off(v))


def attend_kernel(s_ref, cache_ref, draft_ref, mine_ref, other_ref, kv_ref, dk_ref, dv_ref, o_ref):
    cache_len = cache_ref[s_ref[3]]
    draft_len = draft_ref[(s_ref[0] * NY + s_ref[1]) * 2 + s_ref[3]]
    keys = kv_ref[:, 0].reshape(2048, HEAD_DIM)
    values = kv_ref[:, 1].reshape(2048, HEAD_DIM)
    dk = dk_ref[...]
    dv = dv_ref[...]
    keep = lax.broadcasted_iota(jnp.int32, (1, 2048), 1) < cache_len
    row = lax.broadcasted_iota(jnp.int32, (256, DRAFT), 0) % DRAFT
    slot = lax.broadcasted_iota(jnp.int32, (256, DRAFT), 1)
    keep_draft = (slot <= row) & (slot < draft_len)
    live = lax.broadcasted_iota(jnp.int32, (256, 1), 0) % DRAFT < draft_len
    for side, q_ref in enumerate((mine_ref, other_ref)):
        q = jnp.concatenate([q_ref[:, h * HEAD_DIM : (h + 1) * HEAD_DIM] for h in range(4)], axis=0)
        cached = lax.dot_general(q, keys, NT, preferred_element_type=F32)
        drafted = lax.dot_general(q, dk, NT, preferred_element_type=F32)
        cached = jnp.where(keep, cached, NEG_FILL)
        drafted = jnp.where(keep_draft, drafted, NEG_FILL)
        high = jnp.maximum(
            jnp.max(cached, axis=1, keepdims=True), jnp.max(drafted, axis=1, keepdims=True)
        )
        cached = jnp.exp2((cached - high) * EXP2_SCALE)
        drafted = jnp.exp2((drafted - high) * EXP2_SCALE)
        total = jnp.sum(cached, axis=1, keepdims=True) + jnp.sum(drafted, axis=1, keepdims=True)
        mixed = jnp.dot(cached.astype(BF16), values, preferred_element_type=F32)
        mixed = mixed + jnp.dot(drafted.astype(BF16), dv, preferred_element_type=F32)
        mixed = jnp.where(live, mixed / total, 0.0).astype(BF16)
        for h in range(4):
            o_ref[side, :, h * HEAD_DIM : (h + 1) * HEAD_DIM] = mixed[h * DRAFT : (h + 1) * DRAFT]


def attend(ids, cache_lengths, draft_lengths, q, other_q, kv, dk, dv):
    draft = pl.BlockSpec((DRAFT, HEAD_DIM), lambda p, s, *_: (s[3], s[2]))
    return pl.pallas_call(
        attend_kernel,
        grid_spec=pltpu.PrefetchScalarGridSpec(
            num_scalar_prefetch=3,
            grid=(2,),
            in_specs=[
                pl.BlockSpec((DRAFT, 512), lambda p, s, *_: (s[3], p)),
                pl.BlockSpec((DRAFT, 512), lambda p, *_: (0, p)),
                pl.BlockSpec((16, 2, 128, 128), lambda p, *_: (0, 0, 0, 0)),
                draft,
                draft,
            ],
            out_specs=pl.BlockSpec((2, DRAFT, 512), lambda p, *_: (0, 0, p)),
        ),
        out_shape=pltpu.VMEM((2, DRAFT, 1024), BF16),
        compiler_params=PARAMS,
        name="attend",
    )(ids, cache_lengths, draft_lengths, far_off(q), other_q, kv, far_off(dk), far_off(dv))


def project_kernel(count, s_ref, *refs):
    rows, weights, o_ref = refs[:count], refs[count:-1], refs[-1]
    width = count * DRAFT
    a = jnp.concatenate([ref[0] for ref in rows], axis=0)
    b = jnp.concatenate([ref[1] for ref in rows], axis=0)
    for i, step in enumerate((0, -1, 1, 2)):
        acc = jnp.dot(a, weights[2 * i][...], preferred_element_type=F32)
        acc = acc + jnp.dot(b, weights[2 * i + 1][...], preferred_element_type=F32)
        acc = acc.astype(BF16).T.reshape(NZ, 2, 32, width)
        at = lax.rem(s_ref[0] + step + NX, NX)
        for half in range(2):
            o_ref[at, :, :, half * width : (half + 1) * width] = acc[:, half]


def project(ids, rows, weights):
    count = len(rows)
    return pl.pallas_call(
        lambda *refs: project_kernel(count, *refs),
        in_specs=[SMEM] + [VMEM] * (count + 8),
        out_specs=VMEM,
        out_shape=pltpu.VMEM((NX, NZ, 32, 2 * count * DRAFT), BF16),
        compiler_params=PARAMS,
        name="project",
    )(ids, *map(near, rows), *map(near, weights))


def place_kernel(s_ref, length_ref, group_ref, first_ref, *refs):
    parts, o_ref, f_ref = refs[:-2], refs[-2], refs[-1]
    f_ref[...] = jnp.zeros(f_ref.shape, F32)
    my_y, core = s_ref[1], s_ref[3]
    lane = lax.broadcasted_iota(jnp.int32, (32, 128), 1)
    for x in range(NX):
        for slots, ref in zip(CHUNKS, parts):
            width = len(slots) * DRAFT
            for tile in range(2 * width // 128):
                slab = ref[x, 0, :, tile * 128 : (tile + 1) * 128].astype(F32)
                for z in range(1, NZ):
                    slab = slab + ref[x, z, :, tile * 128 : (tile + 1) * 128].astype(F32)
                for part in range(2):
                    column, at = divmod(2 * tile + part, len(slots))
                    request = (x * NY + lax.rem(my_y + slots[at] + NY, NY)) * 2 + core
                    length, group, first = length_ref[request], group_ref[request], first_ref[request]
                    moved = pltpu.roll(slab, lax.rem(first + 64 * part, 128), 1)
                    keep = (lane >= first) & (lane < first + length)
                    spot = 2 * group + column
                    f_ref[spot] = f_ref[spot] + jnp.where(keep, moved, 0.0)
    for t in range(16):
        a, b, c, d = (f_ref[4 * t + i] for i in range(4))
        b, c, d = pltpu.roll(b, 96, 1), pltpu.roll(c, 64, 1), pltpu.roll(d, 32, 1)
        o_ref[t, :, :128] = jnp.where(lane < 96, a, b).astype(BF16)
        o_ref[t, :, 128:256] = jnp.where(lane < 64, b, c).astype(BF16)
        o_ref[t, :, 256:] = jnp.where(lane < 32, c, d).astype(BF16)


def place(tables, parts):
    return pl.pallas_call(
        place_kernel,
        in_specs=[SMEM] * len(tables) + [VMEM] * len(parts),
        out_specs=VMEM,
        out_shape=pltpu.VMEM((16, 32, 4 * PACK), BF16),
        scratch_shapes=[pltpu.VMEM((64, 32, 128), F32)],
        compiler_params=PARAMS,
        name="place",
    )(*tables, *map(near, parts))


def finish_kernel(i_ref, o_ref):
    lane = lax.broadcasted_iota(jnp.int32, (32, 128), 1)
    blocks = [[], []]
    for z in range(NZ):
        v = i_ref[2 * z].astype(F32) + i_ref[2 * z + 1].astype(F32)
        v = [v[:, i * 128 : (i + 1) * 128] for i in range(3)]
        blocks[0].append(v[0])
        blocks[0].append(pltpu.roll(jnp.where(lane < 64, v[1], v[0]), 32, 1))
        blocks[1].append(pltpu.roll(jnp.where(lane < 32, v[2], v[1]), 64, 1))
        blocks[1].append(pltpu.roll(v[2], 96, 1))
    for g in range(2):
        block = jnp.concatenate(blocks[g], axis=0).astype(BF16).T
        o_ref[g * PACK : (g + 1) * PACK] = block[:PACK]


def finish(parts):
    return pl.pallas_call(
        finish_kernel,
        in_specs=[VMEM],
        out_specs=VMEM,
        out_shape=jax.ShapeDtypeStruct((2 * PACK, 512), BF16),
        compiler_params=PARAMS,
        name="finish",
    )(near(parts))


def exchange(value, axes):
    return lax.all_to_all(value, axes, 0, 0, tiled=True)


def layer(
    queries,
    draft_keys,
    draft_values,
    cache_keys,
    cache_values,
    out_weight,
    cache_lengths,
    draft_lengths,
    dest_group,
    dest_offset,
):
    c = lax.axis_index("c")
    ids = jnp.stack([lax.axis_index(name) for name in ("x", "y", "z", "c")]).astype(jnp.int32)

    kv = exchange(pack_kv(cache_keys, cache_values).reshape(16, 2, 128, 128), ("z", "c"))

    w1, w2 = shift(out_weight, "x", NX, 1), shift(out_weight, "x", NX, -1)
    w3 = shift_cores(out_weight, "x", NX, 2)
    weights = []
    for w in (out_weight, w1, w2, w3):
        weights += [w, shift(w, "c", 2, 1)]
    other_q = lax.dynamic_slice_in_dim(queries, (1 - c) * DRAFT, DRAFT, 0)
    other_q = shift(other_q, "c", 2, 1)

    rows = attend(ids, cache_lengths, draft_lengths, queries, other_q, kv, draft_keys, draft_values)
    up1, down1 = shift(rows, "y", NY, 1), shift(rows, "y", NY, -1)
    up2, down2 = shift(rows, "y", NY, 2), shift(rows, "y", NY, -2)
    up3, down3 = shift(up2, "y", NY, 1), shift(down2, "y", NY, -1)
    far = shift_cores(jnp.where(c == 0, up2, down2), "y", NY, 2)
    arrived = {0: rows, -1: up1, 1: down1, -2: up2, 2: down2, -3: up3, 3: down3, -4: far}

    sums = []
    for slots in CHUNKS:
        part = project(ids, [arrived[s] for s in slots], weights)
        part = part.reshape(NX * NZ, 32, -1)
        sums.append(exchange(part, ("x", "z")).reshape(NX, NZ, 32, -1))
    placed = place([ids, draft_lengths, dest_group, dest_offset], sums)
    return finish(exchange(placed, ("z", "c")))


def solution(mesh):
    fine = Mesh(mesh.devices.reshape(NX, NY, NZ, 2), ("x", "y", "z", "c"))
    xy, zc = ("x", "y"), ("z", "c")
    in_specs = (
        P(xy, zc),
        P(xy, None),
        P(xy, None),
        P(xy, zc, None),
        P(xy, zc, None),
        P(zc, xy),
        P(xy),
        P(),
        P(),
        P(),
    )
    return jax.shard_map(layer, mesh=fine, in_specs=in_specs, out_specs=P(zc, xy), check_vma=False)
```

```python
import jax
import jax.numpy as jnp
from jax import lax
from jax.experimental import pallas as pl
from jax.experimental.pallas import tpu as pltpu
from jax.sharding import Mesh, PartitionSpec as P


HEAD_DIM = 128
DRAFT = 64
PACK = 96
NX, NY, NZ = 4, 8, 8
NEG_FILL = -1e30
EXP2_SCALE = HEAD_DIM ** (-0.5) * 1.4426950408889634
BF16 = jnp.bfloat16
F32 = jnp.float32
NT = (((1,), (1,)), ((), ()))
VMEM = pl.BlockSpec(memory_space=pltpu.VMEM)
SMEM = pl.BlockSpec(memory_space=pltpu.SMEM)
PARAMS = pltpu.CompilerParams(vmem_limit_bytes=24 * 2**20)

CHUNKS = ((0, -1, 1, -2, 2), (-3, 3, -4))


def shift(value, axis, size, step):
    return lax.ppermute(value, axis, [(i, (i + step) % size) for i in range(size)])


def shift_cores(value, axis, size, step):
    pairs = [(2 * i + c, 2 * ((i + step * (1 - 2 * c)) % size) + c) for i in range(size) for c in (0, 1)]
    return lax.ppermute(value, (axis, "c"), pairs)


def near(value):
    return pltpu.with_memory_space_constraint(value, pltpu.VMEM)


def far_off(value):
    return pltpu.with_memory_space_constraint(value, pltpu.HBM)


def kv_kernel(k_ref, v_ref, o_ref):
    for h in range(NZ):
        o_ref[h, 0, 0] = k_ref[0, :, h * HEAD_DIM : (h + 1) * HEAD_DIM]
        o_ref[h, 0, 1] = v_ref[0, :, h * HEAD_DIM : (h + 1) * HEAD_DIM]


def pack_kv(k, v):
    return pl.pallas_call(
        kv_kernel,
        grid=(2,),
        in_specs=[pl.BlockSpec((1, 128, 1024), lambda r: (r, 0, 0))] * 2,
        out_specs=pl.BlockSpec((NZ, 1, 2, 128, 128), lambda r: (0, r, 0, 0, 0)),
        out_shape=pltpu.VMEM((NZ, 2, 2, 128, 128), BF16),
        compiler_params=PARAMS,
        name="pack_kv",
    )(far_off(k), far_off(v))


def attend_kernel(s_ref, cache_ref, draft_ref, mine_ref, other_ref, kv_ref, dk_ref, dv_ref, o_ref):
    cache_len = cache_ref[s_ref[3]]
    draft_len = draft_ref[(s_ref[0] * NY + s_ref[1]) * 2 + s_ref[3]]
    keys = kv_ref[:, 0].reshape(2048, HEAD_DIM)
    values = kv_ref[:, 1].reshape(2048, HEAD_DIM)
    dk = dk_ref[...]
    dv = dv_ref[...]
    keep = lax.broadcasted_iota(jnp.int32, (1, 2048), 1) < cache_len
    row = lax.broadcasted_iota(jnp.int32, (256, DRAFT), 0) % DRAFT
    slot = lax.broadcasted_iota(jnp.int32, (256, DRAFT), 1)
    keep_draft = (slot <= row) & (slot < draft_len)
    live = lax.broadcasted_iota(jnp.int32, (256, 1), 0) % DRAFT < draft_len
    for side, q_ref in enumerate((mine_ref, other_ref)):
        q = jnp.concatenate([q_ref[:, h * HEAD_DIM : (h + 1) * HEAD_DIM] for h in range(4)], axis=0)
        cached = lax.dot_general(q, keys, NT, preferred_element_type=F32)
        drafted = lax.dot_general(q, dk, NT, preferred_element_type=F32)
        cached = jnp.where(keep, cached, NEG_FILL)
        drafted = jnp.where(keep_draft, drafted, NEG_FILL)
        high = jnp.maximum(
            jnp.max(cached, axis=1, keepdims=True), jnp.max(drafted, axis=1, keepdims=True)
        )
        cached = jnp.exp2((cached - high) * EXP2_SCALE)
        drafted = jnp.exp2((drafted - high) * EXP2_SCALE)
        total = jnp.sum(cached, axis=1, keepdims=True) + jnp.sum(drafted, axis=1, keepdims=True)
        mixed = jnp.dot(cached.astype(BF16), values, preferred_element_type=F32)
        mixed = mixed + jnp.dot(drafted.astype(BF16), dv, preferred_element_type=F32)
        mixed = jnp.where(live, mixed / total, 0.0).astype(BF16)
        for h in range(4):
            o_ref[side, :, h * HEAD_DIM : (h + 1) * HEAD_DIM] = mixed[h * DRAFT : (h + 1) * DRAFT]


def attend(ids, cache_lengths, draft_lengths, q, other_q, kv, dk, dv):
    draft = pl.BlockSpec((DRAFT, HEAD_DIM), lambda p, s, *_: (s[3], s[2]))
    return pl.pallas_call(
        attend_kernel,
        grid_spec=pltpu.PrefetchScalarGridSpec(
            num_scalar_prefetch=3,
            grid=(2,),
            in_specs=[
                pl.BlockSpec((DRAFT, 512), lambda p, s, *_: (s[3], p)),
                pl.BlockSpec((DRAFT, 512), lambda p, *_: (0, p)),
                pl.BlockSpec((16, 2, 128, 128), lambda p, *_: (0, 0, 0, 0)),
                draft,
                draft,
            ],
            out_specs=pl.BlockSpec((2, DRAFT, 512), lambda p, *_: (0, 0, p)),
        ),
        out_shape=pltpu.VMEM((2, DRAFT, 1024), BF16),
        compiler_params=PARAMS,
        name="attend",
    )(ids, cache_lengths, draft_lengths, far_off(q), other_q, kv, far_off(dk), far_off(dv))


def project_kernel(count, s_ref, *refs):
    rows, weights, o_ref = refs[:count], refs[count:-1], refs[-1]
    width = count * DRAFT
    a = jnp.concatenate([ref[0] for ref in rows], axis=0)
    b = jnp.concatenate([ref[1] for ref in rows], axis=0)
    for i, step in enumerate((0, -1, 1, 2)):
        acc = jnp.dot(a, weights[2 * i][...], preferred_element_type=F32)
        acc = acc + jnp.dot(b, weights[2 * i + 1][...], preferred_element_type=F32)
        acc = acc.astype(BF16).T.reshape(NZ, 2, 32, width)
        at = lax.rem(s_ref[0] + step + NX, NX)
        for half in range(2):
            o_ref[:, at, :, half * width : (half + 1) * width] = acc[:, half]


def project(ids, rows, weights):
    count = len(rows)
    return pl.pallas_call(
        lambda *refs: project_kernel(count, *refs),
        in_specs=[SMEM] + [VMEM] * (count + 8),
        out_specs=VMEM,
        out_shape=pltpu.VMEM((NZ, NX, 32, 2 * count * DRAFT), BF16),
        compiler_params=PARAMS,
        name="project",
    )(ids, *map(near, rows), *map(near, weights))


def place_kernel(s_ref, length_ref, group_ref, first_ref, *refs):
    parts, o_ref, f_ref = refs[:-2], refs[-2], refs[-1]
    f_ref[...] = jnp.zeros(f_ref.shape, F32)
    my_y, core = s_ref[1], s_ref[3]
    lane = lax.broadcasted_iota(jnp.int32, (32, 128), 1)
    for x in range(NX):
        for slots, ref in zip(CHUNKS, parts):
            width = len(slots) * DRAFT
            for tile in range(2 * width // 128):
                slab = ref[0, x, :, tile * 128 : (tile + 1) * 128].astype(F32)
                for z in range(1, NZ):
                    slab = slab + ref[z, x, :, tile * 128 : (tile + 1) * 128].astype(F32)
                for part in range(2):
                    column, at = divmod(2 * tile + part, len(slots))
                    request = (x * NY + lax.rem(my_y + slots[at] + NY, NY)) * 2 + core
                    length, group, first = length_ref[request], group_ref[request], first_ref[request]
                    moved = pltpu.roll(slab, lax.rem(first + 64 * part, 128), 1)
                    keep = (lane >= first) & (lane < first + length)
                    spot = 2 * group + column
                    f_ref[spot] = f_ref[spot] + jnp.where(keep, moved, 0.0)
    for t in range(16):
        a, b, c, d = (f_ref[4 * t + i] for i in range(4))
        b, c, d = pltpu.roll(b, 96, 1), pltpu.roll(c, 64, 1), pltpu.roll(d, 32, 1)
        o_ref[t, :, :128] = jnp.where(lane < 96, a, b).astype(BF16)
        o_ref[t, :, 128:256] = jnp.where(lane < 64, b, c).astype(BF16)
        o_ref[t, :, 256:] = jnp.where(lane < 32, c, d).astype(BF16)


def place(tables, parts):
    return pl.pallas_call(
        place_kernel,
        in_specs=[SMEM] * len(tables) + [VMEM] * len(parts),
        out_specs=VMEM,
        out_shape=pltpu.VMEM((16, 32, 4 * PACK), BF16),
        scratch_shapes=[pltpu.VMEM((64, 32, 128), F32)],
        compiler_params=PARAMS,
        name="place",
    )(*tables, *map(near, parts))


def finish_kernel(i_ref, o_ref):
    lane = lax.broadcasted_iota(jnp.int32, (32, 128), 1)
    blocks = [[], []]
    for z in range(NZ):
        v = i_ref[2 * z].astype(F32) + i_ref[2 * z + 1].astype(F32)
        v = [v[:, i * 128 : (i + 1) * 128] for i in range(3)]
        blocks[0].append(v[0])
        blocks[0].append(pltpu.roll(jnp.where(lane < 64, v[1], v[0]), 32, 1))
        blocks[1].append(pltpu.roll(jnp.where(lane < 32, v[2], v[1]), 64, 1))
        blocks[1].append(pltpu.roll(v[2], 96, 1))
    for g in range(2):
        block = jnp.concatenate(blocks[g], axis=0).astype(BF16).T
        o_ref[g * PACK : (g + 1) * PACK] = block[:PACK]


def finish(parts):
    return pl.pallas_call(
        finish_kernel,
        in_specs=[VMEM],
        out_specs=VMEM,
        out_shape=jax.ShapeDtypeStruct((2 * PACK, 512), BF16),
        compiler_params=PARAMS,
        name="finish",
    )(near(parts))


def exchange(value, axes):
    return lax.all_to_all(value, axes, 0, 0, tiled=True)


def layer(
    queries,
    draft_keys,
    draft_values,
    cache_keys,
    cache_values,
    out_weight,
    cache_lengths,
    draft_lengths,
    dest_group,
    dest_offset,
):
    c = lax.axis_index("c")
    ids = jnp.stack([lax.axis_index(name) for name in ("x", "y", "z", "c")]).astype(jnp.int32)

    kv = exchange(pack_kv(cache_keys, cache_values).reshape(16, 2, 128, 128), ("z", "c"))

    w1, w2 = shift(out_weight, "x", NX, 1), shift(out_weight, "x", NX, -1)
    w3 = shift_cores(out_weight, "x", NX, 2)
    weights = []
    for w in (out_weight, w1, w2, w3):
        weights += [w, shift(w, "c", 2, 1)]
    other_q = lax.dynamic_slice_in_dim(queries, (1 - c) * DRAFT, DRAFT, 0)
    other_q = shift(other_q, "c", 2, 1)

    rows = attend(ids, cache_lengths, draft_lengths, queries, other_q, kv, draft_keys, draft_values)
    up1, down1 = shift(rows, "y", NY, 1), shift(rows, "y", NY, -1)
    up2, down2 = shift(rows, "y", NY, 2), shift(rows, "y", NY, -2)
    up3, down3 = shift(up2, "y", NY, 1), shift(down2, "y", NY, -1)
    far = shift_cores(jnp.where(c == 0, up2, down2), "y", NY, 2)
    arrived = {0: rows, -1: up1, 1: down1, -2: up2, 2: down2, -3: up3, 3: down3, -4: far}

    sums = []
    for slots in CHUNKS:
        part = project(ids, [arrived[s] for s in slots], weights)
        part = part.reshape(NX * NZ, 32, -1)
        sums.append(exchange(part, ("z", "x")).reshape(NZ, NX, 32, -1))
    placed = place([ids, draft_lengths, dest_group, dest_offset], sums)
    return finish(exchange(placed, ("z", "c")))


def solution(mesh):
    fine = Mesh(mesh.devices.reshape(NX, NY, NZ, 2), ("x", "y", "z", "c"))
    xy, zc = ("x", "y"), ("z", "c")
    in_specs = (
        P(xy, zc),
        P(xy, None),
        P(xy, None),
        P(xy, zc, None),
        P(xy, zc, None),
        P(zc, xy),
        P(xy),
        P(),
        P(),
        P(),
    )
    return jax.shard_map(layer, mesh=fine, in_specs=in_specs, out_specs=P(zc, xy), check_vma=False)
```

```python
import jax
import jax.numpy as jnp
from jax import lax
from jax.experimental import pallas as pl
from jax.experimental.pallas import tpu as pltpu
from jax.sharding import Mesh, PartitionSpec as P


HEAD_DIM = 128
DRAFT = 64
PACK = 96
NX, NY, NZ = 4, 8, 8
NEG_FILL = -1e30
EXP2_SCALE = HEAD_DIM ** (-0.5) * 1.4426950408889634
BF16 = jnp.bfloat16
F32 = jnp.float32
NT = (((1,), (1,)), ((), ()))
VMEM = pl.BlockSpec(memory_space=pltpu.VMEM)
SMEM = pl.BlockSpec(memory_space=pltpu.SMEM)
PARAMS = pltpu.CompilerParams(vmem_limit_bytes=24 * 2**20)

CHUNKS = ((0, -1, 1, -2, 2), (-3, 3, -4))


def shift(value, axis, size, step):
    return lax.ppermute(value, axis, [(i, (i + step) % size) for i in range(size)])


def shift_cores(value, axis, size, step):
    pairs = [(2 * i + c, 2 * ((i + step * (1 - 2 * c)) % size) + c) for i in range(size) for c in (0, 1)]
    return lax.ppermute(value, (axis, "c"), pairs)


def near(value):
    return pltpu.with_memory_space_constraint(value, pltpu.VMEM)


def far_off(value):
    return pltpu.with_memory_space_constraint(value, pltpu.HBM)


def kv_kernel(k_ref, v_ref, o_ref):
    for h in range(NZ):
        o_ref[h, 0, 0] = k_ref[0, :, h * HEAD_DIM : (h + 1) * HEAD_DIM]
        o_ref[h, 0, 1] = v_ref[0, :, h * HEAD_DIM : (h + 1) * HEAD_DIM]


def pack_kv(k, v):
    return pl.pallas_call(
        kv_kernel,
        grid=(2,),
        in_specs=[pl.BlockSpec((1, 128, 1024), lambda r: (r, 0, 0))] * 2,
        out_specs=pl.BlockSpec((NZ, 1, 2, 128, 128), lambda r: (0, r, 0, 0, 0)),
        out_shape=pltpu.VMEM((NZ, 2, 2, 128, 128), BF16),
        compiler_params=PARAMS,
        name="pack_kv",
    )(far_off(k), far_off(v))


def attend_kernel(s_ref, cache_ref, draft_ref, mine_ref, other_ref, kv_ref, dk_ref, dv_ref, o_ref):
    cache_len = cache_ref[s_ref[3]]
    draft_len = draft_ref[(s_ref[0] * NY + s_ref[1]) * 2 + s_ref[3]]
    keys = kv_ref[:, 0].reshape(2048, HEAD_DIM)
    values = kv_ref[:, 1].reshape(2048, HEAD_DIM)
    dk = dk_ref[...]
    dv = dv_ref[...]
    keep = lax.broadcasted_iota(jnp.int32, (1, 2048), 1) < cache_len
    row = lax.broadcasted_iota(jnp.int32, (256, DRAFT), 0) % DRAFT
    slot = lax.broadcasted_iota(jnp.int32, (256, DRAFT), 1)
    keep_draft = (slot <= row) & (slot < draft_len)
    live = lax.broadcasted_iota(jnp.int32, (256, 1), 0) % DRAFT < draft_len
    for block in range(4):
        side, q_ref = block // 2, (mine_ref, other_ref)[block // 2]
        columns = [slice(h * HEAD_DIM, (h + 1) * HEAD_DIM) for h in range(4 * (block % 2), 4 * (block % 2) + 4)]
        q = jnp.concatenate([q_ref[:, at] for at in columns], axis=0)
        cached = lax.dot_general(q, keys, NT, preferred_element_type=F32)
        drafted = lax.dot_general(q, dk, NT, preferred_element_type=F32)
        cached = jnp.where(keep, cached, NEG_FILL)
        drafted = jnp.where(keep_draft, drafted, NEG_FILL)
        high = jnp.maximum(
            jnp.max(cached, axis=1, keepdims=True), jnp.max(drafted, axis=1, keepdims=True)
        )
        cached = jnp.exp2((cached - high) * EXP2_SCALE)
        drafted = jnp.exp2((drafted - high) * EXP2_SCALE)
        total = jnp.sum(cached, axis=1, keepdims=True) + jnp.sum(drafted, axis=1, keepdims=True)
        mixed = jnp.dot(cached.astype(BF16), values, preferred_element_type=F32)
        mixed = mixed + jnp.dot(drafted.astype(BF16), dv, preferred_element_type=F32)
        mixed = jnp.where(live, mixed / total, 0.0).astype(BF16)
        for h, at in enumerate(columns):
            o_ref[side, :, at] = mixed[h * DRAFT : (h + 1) * DRAFT]


def attend(ids, cache_lengths, draft_lengths, q, other_q, kv, dk, dv):
    draft = pl.BlockSpec((DRAFT, HEAD_DIM), lambda p, s, *_: (s[3], s[2]))
    return pl.pallas_call(
        attend_kernel,
        grid_spec=pltpu.PrefetchScalarGridSpec(
            num_scalar_prefetch=3,
            grid=(1,),
            in_specs=[
                pl.BlockSpec((DRAFT, 1024), lambda p, s, *_: (s[3], p)),
                pl.BlockSpec((DRAFT, 1024), lambda p, *_: (0, p)),
                pl.BlockSpec((16, 2, 128, 128), lambda p, *_: (0, 0, 0, 0)),
                draft,
                draft,
            ],
            out_specs=pl.BlockSpec((2, DRAFT, 1024), lambda p, *_: (0, 0, p)),
        ),
        out_shape=pltpu.VMEM((2, DRAFT, 1024), BF16),
        compiler_params=PARAMS,
        name="attend",
    )(ids, cache_lengths, draft_lengths, far_off(q), other_q, kv, far_off(dk), far_off(dv))


def project_kernel(count, s_ref, *refs):
    rows, weights, o_ref = refs[:count], refs[count:-1], refs[-1]
    width = count * DRAFT
    a = jnp.concatenate([ref[0] for ref in rows], axis=0)
    b = jnp.concatenate([ref[1] for ref in rows], axis=0)
    for i, step in enumerate((0, -1, 1, 2)):
        acc = jnp.dot(a, weights[2 * i][...], preferred_element_type=F32)
        acc = acc + jnp.dot(b, weights[2 * i + 1][...], preferred_element_type=F32)
        acc = acc.astype(BF16).T.reshape(NZ, 2, 32, width)
        at = lax.rem(s_ref[0] + step + NX, NX)
        for half in range(2):
            o_ref[:, at, :, half * width : (half + 1) * width] = acc[:, half]


def project(ids, rows, weights):
    count = len(rows)
    return pl.pallas_call(
        lambda *refs: project_kernel(count, *refs),
        in_specs=[SMEM] + [VMEM] * (count + 8),
        out_specs=VMEM,
        out_shape=pltpu.VMEM((NZ, NX, 32, 2 * count * DRAFT), BF16),
        compiler_params=PARAMS,
        name="project",
    )(ids, *map(near, rows), *map(near, weights))


def place_kernel(s_ref, length_ref, group_ref, first_ref, *refs):
    parts, o_ref, f_ref = refs[:-2], refs[-2], refs[-1]
    f_ref[...] = jnp.zeros(f_ref.shape, F32)
    my_y, core = s_ref[1], s_ref[3]
    lane = lax.broadcasted_iota(jnp.int32, (32, 128), 1)
    for x in range(NX):
        for slots, ref in zip(CHUNKS, parts):
            width = len(slots) * DRAFT
            for tile in range(2 * width // 128):
                slab = ref[0, x, :, tile * 128 : (tile + 1) * 128].astype(F32)
                for z in range(1, NZ):
                    slab = slab + ref[z, x, :, tile * 128 : (tile + 1) * 128].astype(F32)
                for part in range(2):
                    column, at = divmod(2 * tile + part, len(slots))
                    request = (x * NY + lax.rem(my_y + slots[at] + NY, NY)) * 2 + core
                    length, group, first = length_ref[request], group_ref[request], first_ref[request]
                    moved = pltpu.roll(slab, lax.rem(first + 64 * part, 128), 1)
                    keep = (lane >= first) & (lane < first + length)
                    spot = 2 * group + column
                    f_ref[spot] = f_ref[spot] + jnp.where(keep, moved, 0.0)
    for t in range(16):
        a, b, c, d = (f_ref[4 * t + i] for i in range(4))
        b, c, d = pltpu.roll(b, 96, 1), pltpu.roll(c, 64, 1), pltpu.roll(d, 32, 1)
        o_ref[t, :, :128] = jnp.where(lane < 96, a, b).astype(BF16)
        o_ref[t, :, 128:256] = jnp.where(lane < 64, b, c).astype(BF16)
        o_ref[t, :, 256:] = jnp.where(lane < 32, c, d).astype(BF16)


def place(tables, parts):
    return pl.pallas_call(
        place_kernel,
        in_specs=[SMEM] * len(tables) + [VMEM] * len(parts),
        out_specs=VMEM,
        out_shape=pltpu.VMEM((16, 32, 4 * PACK), BF16),
        scratch_shapes=[pltpu.VMEM((64, 32, 128), F32)],
        compiler_params=PARAMS,
        name="place",
    )(*tables, *map(near, parts))


def finish_kernel(i_ref, o_ref):
    lane = lax.broadcasted_iota(jnp.int32, (32, 128), 1)
    blocks = [[], []]
    for z in range(NZ):
        v = i_ref[2 * z].astype(F32) + i_ref[2 * z + 1].astype(F32)
        v = [v[:, i * 128 : (i + 1) * 128] for i in range(3)]
        blocks[0].append(v[0])
        blocks[0].append(pltpu.roll(jnp.where(lane < 64, v[1], v[0]), 32, 1))
        blocks[1].append(pltpu.roll(jnp.where(lane < 32, v[2], v[1]), 64, 1))
        blocks[1].append(pltpu.roll(v[2], 96, 1))
    for g in range(2):
        block = jnp.concatenate(blocks[g], axis=0).astype(BF16).T
        o_ref[g * PACK : (g + 1) * PACK] = block[:PACK]


def finish(parts):
    return pl.pallas_call(
        finish_kernel,
        in_specs=[VMEM],
        out_specs=VMEM,
        out_shape=jax.ShapeDtypeStruct((2 * PACK, 512), BF16),
        compiler_params=PARAMS,
        name="finish",
    )(near(parts))


def exchange(value, axes):
    return lax.all_to_all(value, axes, 0, 0, tiled=True)


def layer(
    queries,
    draft_keys,
    draft_values,
    cache_keys,
    cache_values,
    out_weight,
    cache_lengths,
    draft_lengths,
    dest_group,
    dest_offset,
):
    c = lax.axis_index("c")
    ids = jnp.stack([lax.axis_index(name) for name in ("x", "y", "z", "c")]).astype(jnp.int32)

    kv = exchange(pack_kv(cache_keys, cache_values).reshape(16, 2, 128, 128), ("z", "c"))

    w1, w2 = shift(out_weight, "x", NX, 1), shift(out_weight, "x", NX, -1)
    w3 = shift_cores(out_weight, "x", NX, 2)
    weights = []
    for w in (out_weight, w1, w2, w3):
        weights += [w, shift(w, "c", 2, 1)]
    other_q = lax.dynamic_slice_in_dim(queries, (1 - c) * DRAFT, DRAFT, 0)
    other_q = shift(other_q, "c", 2, 1)

    rows = attend(ids, cache_lengths, draft_lengths, queries, other_q, kv, draft_keys, draft_values)
    up1, down1 = shift(rows, "y", NY, 1), shift(rows, "y", NY, -1)
    up2, down2 = shift(rows, "y", NY, 2), shift(rows, "y", NY, -2)
    up3, down3 = shift(up2, "y", NY, 1), shift(down2, "y", NY, -1)
    far = shift_cores(jnp.where(c == 0, up2, down2), "y", NY, 2)
    arrived = {0: rows, -1: up1, 1: down1, -2: up2, 2: down2, -3: up3, 3: down3, -4: far}

    sums = []
    for slots in CHUNKS:
        part = project(ids, [arrived[s] for s in slots], weights)
        part = part.reshape(NX * NZ, 32, -1)
        sums.append(exchange(part, ("z", "x")).reshape(NZ, NX, 32, -1))
    placed = place([ids, draft_lengths, dest_group, dest_offset], sums)
    return finish(exchange(placed, ("z", "c")))


def solution(mesh):
    fine = Mesh(mesh.devices.reshape(NX, NY, NZ, 2), ("x", "y", "z", "c"))
    xy, zc = ("x", "y"), ("z", "c")
    in_specs = (
        P(xy, zc),
        P(xy, None),
        P(xy, None),
        P(xy, zc, None),
        P(xy, zc, None),
        P(zc, xy),
        P(xy),
        P(),
        P(),
        P(),
    )
    return jax.shard_map(layer, mesh=fine, in_specs=in_specs, out_specs=P(zc, xy), check_vma=False)
```
